32 devices in a mesh: rep: 2 (over x), ep: 4 (over z), fsdp: 4 (over y, core).
Axes of the slice: x: 2, y: 2, z: 4, core: 2. Of those that a mesh axis runs over, the one named last changes fastest.
Arguments:
- x_in: bfloat16 [8192, 4096], P(('rep', 'ep', 'fsdp')), parts along dimension 0
- norm_w: float32 [2, 4096], replicated
- router_w: bfloat16 [2, 4096, 8], replicated
- gate_w: bfloat16 [2, 8, 4096, 1376], P(None, 'ep', None, 'fsdp')
- up_w: bfloat16 [2, 8, 4096, 1376], P(None, 'ep', None, 'fsdp')
- down_w: bfloat16 [2, 8, 1376, 4096], P(None, 'ep', 'fsdp')
- routes: int32 [2, 8192, 2], P(None, ('rep', 'ep', 'fsdp')), parts along dimension 1
Outputs:
- output: bfloat16 [8192, 4096], P(('rep', 'ep', 'fsdp')), parts along dimension 0
There are 2 independent parts. The reference program is written for one: setup_inputs(seed, part) draws one part's arguments, and reference() takes and returns one part's arrays. A program takes and returns all parts, laid end to end along the dimension named above; an argument that names none is the same for every part.
All inputs are finite; a program needn't handle non-finite values.
Results may differ from the reference program's by a relative error of at most 0.0123691.
Values are sent between devices in bfloat16 or wider.
A program may use at most 1 GiB of HBM per device.

```python
import jax
import jax.numpy as jnp
from jax import lax
import numpy as np

EXPERTS = 8
TOP = 2
D_MODEL = 4096
FF_DIM = 1376
TOK_DEV = 256
DEV_PART = 16
LAYERS = 2

NORM_EPS = 1e-5
CAPACITY = 8 * ((2 * TOK_DEV * TOP + 8 * EXPERTS - 1) // (8 * EXPERTS))
TOKENS = TOK_DEV * DEV_PART
ROW_CAP = DEV_PART * CAPACITY


def count_pattern(n_pairs, n_experts, capacity):
    counts = [1 + ((capacity - 1) * (n_experts - 1 - position)) // (n_experts - 1) for position in range(n_experts)]
    cursor = 1
    while sum(counts) < n_pairs:
        if counts[cursor] < capacity:
            counts[cursor] += 1
        cursor = cursor % (n_experts - 1) + 1
    while sum(counts) > n_pairs:
        if counts[cursor] > 1:
            counts[cursor] -= 1
        cursor = cursor % (n_experts - 1) + 1
    return counts


def draw_routes(route_key):
    counts = count_pattern(TOK_DEV * TOP, EXPERTS, CAPACITY)
    pattern = np.repeat(np.arange(EXPERTS), counts).astype(np.int32)

    def one_block(block_key):
        key_label, key_order = jax.random.split(block_key)
        relabel = jax.random.permutation(key_label, EXPERTS)
        expert_ids = relabel[pattern].reshape(TOP, TOK_DEV).T
        token_order = jax.random.permutation(key_order, TOK_DEV)
        return expert_ids[token_order]

    block_keys = jax.random.split(route_key, LAYERS * DEV_PART)
    all_blocks = jax.vmap(one_block)(block_keys)
    return all_blocks.reshape(LAYERS, TOKENS, TOP).astype(jnp.int32)


def setup_inputs(seed: int = 0, part: int = 0) -> dict:
    weight_keys = jax.random.split(jax.random.key(seed), 5)
    part_keys = jax.random.split(jax.random.fold_in(jax.random.key(seed + 1), part), 2)
    x_in = jax.random.normal(part_keys[0], (TOKENS, D_MODEL), jnp.float32).astype(jnp.bfloat16)
    norm_w = 1.0 + 0.25 * jax.random.normal(weight_keys[0], (LAYERS, D_MODEL), jnp.float32)
    router_w = (jax.random.normal(weight_keys[1], (LAYERS, D_MODEL, EXPERTS), jnp.float32) * D_MODEL ** -0.5).astype(jnp.bfloat16)
    gate_w = (jax.random.normal(weight_keys[2], (LAYERS, EXPERTS, D_MODEL, FF_DIM), jnp.float32) * D_MODEL ** -0.5).astype(jnp.bfloat16)
    up_w = (jax.random.normal(weight_keys[3], (LAYERS, EXPERTS, D_MODEL, FF_DIM), jnp.float32) * D_MODEL ** -0.5).astype(jnp.bfloat16)
    down_w = (jax.random.normal(weight_keys[4], (LAYERS, EXPERTS, FF_DIM, D_MODEL), jnp.float32) * (1.5 * (TOP / FF_DIM) ** 0.5)).astype(jnp.bfloat16)
    routes = draw_routes(part_keys[1])
    return {"x_in": x_in, "norm_w": norm_w, "router_w": router_w, "gate_w": gate_w, "up_w": up_w, "down_w": down_w, "routes": routes}


def rms_norm(stream, norm_row):
    widened = stream.astype(jnp.float32)
    inv_rms = lax.rsqrt(jnp.mean(widened * widened, axis=-1, keepdims=True) + NORM_EPS)
    return (widened * inv_rms * norm_row).astype(jnp.bfloat16)


def moe_layer(stream, layer_params):
    norm_row, router_l, gate_l, up_l, down_l, routes_l = layer_params
    hidden = rms_norm(stream, norm_row)
    logits = jnp.dot(hidden, router_l, preferred_element_type=jnp.float32)
    gate_probs = jax.nn.softmax(jnp.take_along_axis(logits, routes_l, axis=1), axis=-1)

    def expert_step(mixed_sum, expert_params):
        expert_id, gate_e, up_e, down_e = expert_params
        is_chosen = routes_l == expert_id
        token_gate = jnp.sum(jnp.where(is_chosen, gate_probs, 0.0), axis=1)
        token_rows = jnp.nonzero(jnp.any(is_chosen, axis=1), size=ROW_CAP, fill_value=0)[0]
        row_valid = jnp.arange(ROW_CAP) < jnp.sum(is_chosen)
        row_gate = jnp.where(row_valid, token_gate[token_rows], 0.0)
        picked = hidden[token_rows]
        pre_gate = jnp.dot(picked, gate_e, preferred_element_type=jnp.float32)
        pre_up = jnp.dot(picked, up_e, preferred_element_type=jnp.float32)
        inner_act = (jax.nn.silu(pre_gate) * pre_up).astype(jnp.bfloat16)
        expert_out = jnp.dot(inner_act, down_e, preferred_element_type=jnp.float32).astype(jnp.bfloat16)
        mixed_sum = mixed_sum.at[token_rows].add(row_gate[:, None] * expert_out.astype(jnp.float32))
        return mixed_sum, None

    start_sum = jnp.zeros(stream.shape, jnp.float32)
    mixed_sum, _ = lax.scan(expert_step, start_sum, (jnp.arange(EXPERTS), gate_l, up_l, down_l))
    return (stream.astype(jnp.float32) + mixed_sum).astype(jnp.bfloat16), None


def reference(x_in, norm_w, router_w, gate_w, up_w, down_w, routes):
    final_stream, _ = lax.scan(moe_layer, x_in, (norm_w, router_w, gate_w, up_w, down_w, routes))
    return final_stream
```

```python
import functools

import jax
import jax.numpy as jnp
from jax import lax
from jax.experimental import pallas as pl
from jax.experimental.pallas import tpu as pltpu
from jax.sharding import PartitionSpec as P

NORM_EPS = 1e-5
ANY = pl.BlockSpec(memory_space=pl.ANY)
VMEM = pl.BlockSpec(memory_space=pltpu.VMEM)
SMEM = pl.BlockSpec(memory_space=pltpu.SMEM)
VMEM_BYTES = 62 * 1024 * 1024
COL_CHUNK = 512


def norm_and_gates(y_f32_of, h_ref, gates_ref, norm_ref, router_ref, routes_ref, rows, width):
    chunks = width // COL_CHUNK
    sq = jnp.zeros((rows, 1), jnp.float32)
    for c in range(chunks):
        y = y_f32_of(c)
        sq += jnp.sum(y * y, axis=1, keepdims=True)
    inv = lax.rsqrt(sq / width + NORM_EPS)
    logits = jnp.zeros((rows, router_ref.shape[1]), jnp.float32)
    for c in range(chunks):
        cols = pl.ds(c * COL_CHUNK, COL_CHUNK)
        h = (y_f32_of(c) * inv * norm_ref[:, cols]).astype(jnp.bfloat16)
        h_ref[:, cols] = h
        logits += jnp.dot(h, router_ref[cols, :], preferred_element_type=jnp.float32)
    ids = lax.broadcasted_iota(jnp.int32, logits.shape, 1)
    picked = [jnp.sum(jnp.where(ids == routes_ref[:, j:j + 1], logits, 0.0), axis=1, keepdims=True) for j in range(2)]
    top = jnp.maximum(picked[0], picked[1])
    e0, e1 = jnp.exp(picked[0] - top), jnp.exp(picked[1] - top)
    gates_ref[:, 0:1] = e0 / (e0 + e1)
    gates_ref[:, 1:2] = e1 / (e0 + e1)


def first_norm_kernel(x_ref, norm_ref, router_ref, routes_ref, h_ref, gates_ref):
    rows, width = x_ref.shape

    def y_of(c):
        return x_ref[:, pl.ds(c * COL_CHUNK, COL_CHUNK)].astype(jnp.float32)

    norm_and_gates(y_of, h_ref, gates_ref, norm_ref, router_ref, routes_ref, rows, width)


def first_norm(x, norm_row, router_l, routes_l):
    rows, width = x.shape
    return pl.pallas_call(
        first_norm_kernel,
        out_shape=(jax.ShapeDtypeStruct((rows, width), jnp.bfloat16), jax.ShapeDtypeStruct((rows, 2), jnp.float32)),
        in_specs=[VMEM] * 4, out_specs=(VMEM, VMEM),
        compiler_params=pltpu.CompilerParams(vmem_limit_bytes=VMEM_BYTES),
        cost_estimate=pl.CostEstimate(flops=4_000_000_000, bytes_accessed=3 * rows * width * 2, transcendentals=0),
        name="first_norm",
    )(x, norm_row, router_l, routes_l)


def combine_kernel(with_norm, n_parts, *refs):
    x_ref, gates_ref, slots_ref = refs[:3]
    parts = refs[3:3 + n_parts]
    rest = refs[3 + n_parts:]
    if with_norm:
        norm_ref, router_ref, routes_ref, y_ref, h_ref, next_gates_ref, back, sems = rest
    else:
        y_ref, back, sems = rest
    rows, width = x_ref.shape
    cap = parts[0].shape[0]
    copies = [pltpu.make_async_copy(parts[p], back.at[pl.ds(p * cap, cap)], sems.at[p]) for p in range(n_parts)]
    for copy in copies:
        copy.start()
    total = n_parts * cap
    ids = lax.broadcasted_iota(jnp.int32, (rows, total), 1)
    pick = [(ids == slots_ref[:, j:j + 1]).astype(jnp.float32).astype(jnp.bfloat16) for j in range(2)]
    for copy in copies:
        copy.wait()
    for c in range(width // COL_CHUNK):
        cols = pl.ds(c * COL_CHUNK, COL_CHUNK)
        mixed = sum(gates_ref[:, j:j + 1] * jnp.dot(pick[j], back[:, cols], preferred_element_type=jnp.float32) for j in range(2))
        y_ref[:, cols] = (x_ref[:, cols].astype(jnp.float32) + mixed).astype(jnp.bfloat16)
    if with_norm:
        def y_of(c):
            return y_ref[:, pl.ds(c * COL_CHUNK, COL_CHUNK)].astype(jnp.float32)

        norm_and_gates(y_of, h_ref, next_gates_ref, norm_ref, router_ref, routes_ref, rows, width)


def combine(x, gates, slots, parts, next_args):
    rows, width = x.shape
    cap, n = parts[0].shape[0], len(parts)
    out_shape = [jax.ShapeDtypeStruct((rows, width), jnp.bfloat16)]
    if next_args:
        out_shape += [jax.ShapeDtypeStruct((rows, width), jnp.bfloat16), jax.ShapeDtypeStruct((rows, 2), jnp.float32)]
    return pl.pallas_call(
        functools.partial(combine_kernel, bool(next_args), n),
        out_shape=tuple(out_shape),
        in_specs=[VMEM] * 3 + [ANY] * n + [VMEM] * len(next_args), out_specs=tuple([VMEM] * len(out_shape)),
        scratch_shapes=[pltpu.VMEM((n * cap, width), jnp.bfloat16), pltpu.SemaphoreType.DMA((n,))],
        compiler_params=pltpu.CompilerParams(vmem_limit_bytes=VMEM_BYTES),
        cost_estimate=pl.CostEstimate(flops=12_000_000_000, bytes_accessed=(n * cap + 3 * rows) * width * 2, transcendentals=0),
        name="combine",
    )(x, gates, slots, *parts, *next_args)


def ffn_kernel(layer, local, n_blocks, *refs):
    half_ref, ranks_ref = refs[:2]
    h_refs = refs[2:2 + n_blocks]
    own_g, own_u, own_d, mate_g, mate_u, mate_d = refs[2 + n_blocks:8 + n_blocks]
    far = refs[8 + n_blocks:16 + n_blocks]
    outs = refs[16 + n_blocks:16 + 2 * n_blocks]
    wg, wu, wd, picked, act, sem_g, sem_u, sem_d = refs[16 + 2 * n_blocks:]
    cap = outs[0].shape[0]
    width = wg.shape[1]
    half = width // 2
    first = half_ref[0]
    lo = pl.multiple_of(first * half, half)
    hi = pl.multiple_of((1 - first) * half, half)

    for f, (g, u, d) in enumerate(((own_g, own_u, own_d), (mate_g, mate_u, mate_d))):
        pltpu.make_async_copy(g.at[layer, local], wg.at[f], sem_g.at[f]).start()
        pltpu.make_async_copy(u.at[layer, local], wu.at[f], sem_u.at[f]).start()
    for f, (a_gu, b_gu, a_d, b_d) in ((2, far[:4]), (3, far[4:])):
        for gu, start in ((a_gu, lo), (b_gu, hi)):
            pltpu.make_async_copy(gu.at[0], wg.at[f, pl.ds(start, half)], sem_g.at[f]).start()
            pltpu.make_async_copy(gu.at[1], wu.at[f, pl.ds(start, half)], sem_u.at[f]).start()
    for f, d in enumerate((own_d, mate_d)):
        pltpu.make_async_copy(d.at[layer, local], wd.at[f], sem_d.at[f]).start()
    for f, (a_gu, b_gu, a_d, b_d) in ((2, far[:4]), (3, far[4:])):
        for d, start in ((a_d, lo), (b_d, hi)):
            pltpu.make_async_copy(d, wd.at[f, :, pl.ds(start, half)], sem_d.at[f]).start()

    for b in range(n_blocks):
        slot = lax.broadcasted_iota(jnp.int32, (cap, ranks_ref.shape[1]), 0)
        pick = (slot == ranks_ref[b:b + 1, :]).astype(jnp.float32).astype(jnp.bfloat16)

        def pick_cols(c, _, b=b, pick=pick):
            cols = pl.ds(pl.multiple_of(c * COL_CHUNK, COL_CHUNK), COL_CHUNK)
            picked[pl.ds(b * cap, cap), cols] = jnp.dot(pick, h_refs[b][:, cols], preferred_element_type=jnp.float32).astype(jnp.bfloat16)
            return _

        lax.fori_loop(0, width // COL_CHUNK, pick_cols, 0)

    def up_step(f, _):
        pltpu.make_async_copy(wg.at[f], wg.at[f], sem_g.at[f]).wait()
        pltpu.make_async_copy(wu.at[f], wu.at[f], sem_u.at[f]).wait()
        pre_gate = jnp.dot(picked[...], wg[f], preferred_element_type=jnp.float32)
        pre_up = jnp.dot(picked[...], wu[f], preferred_element_type=jnp.float32)
        act[f] = (jax.nn.silu(pre_gate) * pre_up).astype(jnp.bfloat16)
        return _

    lax.fori_loop(0, 4, up_step, 0)
    for f in range(4):
        pltpu.make_async_copy(wd.at[f], wd.at[f], sem_d.at[f]).wait()

    def down_step(c, _):
        cols = pl.ds(pl.multiple_of(c * COL_CHUNK, COL_CHUNK), COL_CHUNK)
        total = jnp.dot(act[0], wd[0, :, cols], preferred_element_type=jnp.float32)
        for f in range(1, 4):
            total += jnp.dot(act[f], wd[f, :, cols], preferred_element_type=jnp.float32)
        for b in range(n_blocks):
            outs[b][:, cols] = total[b * cap:(b + 1) * cap].astype(jnp.bfloat16)
        return _

    lax.fori_loop(0, width // COL_CHUNK, down_step, 0)


def ffn(layer, local, cap, half_idx, ranks, blocks, own, mate, far):
    n = len(blocks)
    width = blocks[0].shape[1]
    ff = own[0].shape[3]
    rows = n * cap
    return pl.pallas_call(
        functools.partial(ffn_kernel, layer, local, n),
        out_shape=tuple([jax.ShapeDtypeStruct((cap, width), jnp.bfloat16)] * n),
        in_specs=[SMEM, VMEM] + [VMEM] * n + [ANY] * 14, out_specs=tuple([VMEM] * n),
        scratch_shapes=[pltpu.VMEM((4, width, ff), jnp.bfloat16), pltpu.VMEM((4, width, ff), jnp.bfloat16),
                        pltpu.VMEM((4, ff, width), jnp.bfloat16), pltpu.VMEM((rows, width), jnp.bfloat16),
                        pltpu.VMEM((4, rows, ff), jnp.bfloat16), pltpu.SemaphoreType.DMA((4,)),
                        pltpu.SemaphoreType.DMA((4,)), pltpu.SemaphoreType.DMA((4,))],
        compiler_params=pltpu.CompilerParams(vmem_limit_bytes=VMEM_BYTES),
        cost_estimate=pl.CostEstimate(flops=6 * rows * width * 4 * ff, bytes_accessed=12 * width * ff * 2 + 4 * rows * width * 2, transcendentals=0),
        name="expert_ffn",
    )(half_idx, ranks, *blocks, *own, *mate, *far)


def solution(mesh):
    n_ep, n_fs, n_rep = mesh.shape["ep"], mesh.shape["fsdp"], mesh.shape["rep"]
    token_spec = P(("rep", "ep", "fsdp"), None)
    expert_in_spec = P(None, "ep", None, "fsdp")
    expert_out_spec = P(None, "ep", "fsdp", None)
    route_spec = P(None, ("rep", "ep", "fsdp"), None)
    to_mate = [(f, f ^ 1) for f in range(n_fs)]
    to_far = [(f, f ^ 2) for f in range(n_fs)]
    to_rep = [(r, r ^ 1) for r in range(n_rep)]

    def device_step(x_in, norm_w, router_w, gate_w, up_w, down_w, routes):
        layers, tok_dev, top_k = routes.shape
        n_local = gate_w.shape[1]
        width = x_in.shape[1]
        half = width // 2
        experts = router_w.shape[2]
        cap = tok_dev * top_k // 4
        rep, ep = lax.axis_index("rep"), lax.axis_index("ep")
        half_idx = rep.reshape(1).astype(jnp.int32)

        own = (gate_w, up_w, down_w)
        far = {}
        for l in range(layers):
            for k in range(n_local):
                g_half = lax.dynamic_slice(gate_w, (l, k, rep * half, 0), (1, 1, half, gate_w.shape[3]))
                u_half = lax.dynamic_slice(up_w, (l, k, rep * half, 0), (1, 1, half, up_w.shape[3]))
                d_half = lax.dynamic_slice(down_w, (l, k, 0, rep * half), (1, 1, down_w.shape[2], half))[0, 0]
                gu_half = jnp.concatenate([g_half[0], u_half[0]], axis=0)
                a_gu, a_d = (lax.ppermute(t, "fsdp", to_far) for t in (gu_half, d_half))
                b_gu, b_d = (lax.ppermute(t, "rep", to_rep) for t in (a_gu, a_d))
                mine = (a_gu, b_gu, a_d, b_d)
                far[l, k] = mine + tuple(lax.ppermute(t, "fsdp", to_mate) for t in mine)
        mate = tuple(lax.ppermute(t, "fsdp", to_mate) for t in own)

        all_routes = lax.all_gather(routes, "ep", axis=0)
        local_ids = ep * n_local + jnp.arange(n_local, dtype=jnp.int32)
        before = (jnp.arange(tok_dev)[:, None] < jnp.arange(tok_dev)[None, :]).astype(jnp.bfloat16)

        def rank_of(routes_blt2, ids):
            chosen = jnp.any(routes_blt2[..., None, :, :] == ids[:, None, None], axis=-1)
            rank = jnp.einsum("...t,ts->...s", chosen.astype(jnp.bfloat16), before, preferred_element_type=jnp.float32).astype(jnp.int32)
            return jnp.where(chosen, rank, -1)

        block_order = ep ^ jnp.arange(n_ep, dtype=jnp.int32)
        ranks = rank_of(all_routes[block_order], local_ids)
        own_rank = rank_of(routes, jnp.arange(experts, dtype=jnp.int32))
        pair_rank = jnp.take_along_axis(own_rank, routes.transpose(0, 2, 1), axis=1).transpose(0, 2, 1)
        slots = (((routes // n_local) ^ ep) * n_local + routes % n_local) * cap + pair_rank

        up1 = [(z, z + 1) for z in range(n_ep - 1)]
        down1 = [(z + 1, z) for z in range(n_ep - 1)]
        stream = x_in
        hidden, gates = first_norm(stream, norm_w[0:1], router_w[0], routes[0])
        for l in range(layers):
            lo1 = lax.ppermute(hidden, "ep", up1)
            hi1 = lax.ppermute(hidden, "ep", down1)
            lo2 = lax.ppermute(lo1, "ep", [(1, 2), (2, 3)])
            hi2 = lax.ppermute(hi1, "ep", [(2, 1), (1, 0)])
            lo3 = lax.ppermute(lo2, "ep", [(2, 3)])
            hi3 = lax.ppermute(hi2, "ep", [(1, 0)])
            even = ep % 2 == 0
            q1 = jnp.where(even, hi1, lo1)
            q2 = jnp.where(ep < 2, hi2, lo2)
            q3 = jnp.where(ep == 0, hi3, jnp.where(ep == 1, hi1, jnp.where(ep == 2, lo1, lo3)))
            groups = (((0, 1), (hidden, q1)), ((2,), (q2,)), ((3,), (q3,)))
            parts = {}
            for k in range(n_local):
                for qs, blocks in groups:
                    rank_rows = jnp.stack([ranks[q, l, k] for q in qs])
                    outs = ffn(l, k, cap, half_idx, rank_rows, blocks, own, mate, far[l, k])
                    for q, out in zip(qs, outs):
                        parts[q, k] = out if q == 0 else lax.ppermute(out, "ep", [(z, z ^ q) for z in range(n_ep)])
            ordered = [parts[q, k] for q in range(n_ep) for k in range(n_local)]
            if l + 1 < layers:
                stream, hidden, gates = combine(stream, gates, slots[l], ordered, (norm_w[l + 1:l + 2], router_w[l + 1], routes[l + 1]))
            else:
                stream, = combine(stream, gates, slots[l], ordered, ())
        return stream

    return jax.shard_map(device_step, mesh=mesh,
                         in_specs=(token_spec, P(), P(), expert_in_spec, expert_in_spec, expert_out_spec, route_spec),
                         out_specs=token_spec, check_vma=False)
```

```python
import functools

import jax
import jax.numpy as jnp
from jax import lax
from jax.experimental import pallas as pl
from jax.experimental.pallas import tpu as pltpu
from jax.sharding import PartitionSpec as P

NORM_EPS = 1e-5
ANY = pl.BlockSpec(memory_space=pl.ANY)
VMEM = pl.BlockSpec(memory_space=pltpu.VMEM)
SMEM = pl.BlockSpec(memory_space=pltpu.SMEM)
VMEM_BYTES = 62 * 1024 * 1024
COL_CHUNK = 512


def norm_and_gates(y_f32_of, h_ref, gates_ref, norm_ref, router_ref, routes_ref, rows, width):
    chunks = width // COL_CHUNK
    sq = jnp.zeros((rows, 1), jnp.float32)
    for c in range(chunks):
        y = y_f32_of(c)
        sq += jnp.sum(y * y, axis=1, keepdims=True)
    inv = lax.rsqrt(sq / width + NORM_EPS)
    logits = jnp.zeros((rows, router_ref.shape[1]), jnp.float32)
    for c in range(chunks):
        cols = pl.ds(c * COL_CHUNK, COL_CHUNK)
        h = (y_f32_of(c) * inv * norm_ref[:, cols]).astype(jnp.bfloat16)
        h_ref[:, cols] = h
        logits += jnp.dot(h, router_ref[cols, :], preferred_element_type=jnp.float32)
    ids = lax.broadcasted_iota(jnp.int32, logits.shape, 1)
    picked = [jnp.sum(jnp.where(ids == routes_ref[:, j:j + 1], logits, 0.0), axis=1, keepdims=True) for j in range(2)]
    top = jnp.maximum(picked[0], picked[1])
    e0, e1 = jnp.exp(picked[0] - top), jnp.exp(picked[1] - top)
    gates_ref[:, 0:1] = e0 / (e0 + e1)
    gates_ref[:, 1:2] = e1 / (e0 + e1)


def first_norm_kernel(x_ref, norm_ref, router_ref, routes_ref, h_ref, gates_ref):
    rows, width = x_ref.shape

    def y_of(c):
        return x_ref[:, pl.ds(c * COL_CHUNK, COL_CHUNK)].astype(jnp.float32)

    norm_and_gates(y_of, h_ref, gates_ref, norm_ref, router_ref, routes_ref, rows, width)


def first_norm(x, norm_row, router_l, routes_l):
    rows, width = x.shape
    return pl.pallas_call(
        first_norm_kernel,
        out_shape=(jax.ShapeDtypeStruct((rows, width), jnp.bfloat16), jax.ShapeDtypeStruct((rows, 2), jnp.float32)),
        in_specs=[VMEM] * 4, out_specs=(VMEM, VMEM),
        compiler_params=pltpu.CompilerParams(vmem_limit_bytes=VMEM_BYTES),
        cost_estimate=pl.CostEstimate(flops=4_000_000_000, bytes_accessed=3 * rows * width * 2, transcendentals=0),
        name="first_norm",
    )(x, norm_row, router_l, routes_l)


def combine_kernel(with_norm, n_parts, *refs):
    x_ref, gates_ref, slots_ref = refs[:3]
    parts = refs[3:3 + n_parts]
    rest = refs[3 + n_parts:]
    if with_norm:
        norm_ref, router_ref, routes_ref, y_ref, h_ref, next_gates_ref, back, sems = rest
    else:
        y_ref, back, sems = rest
    rows, width = x_ref.shape
    cap = parts[0].shape[0]
    copies = [pltpu.make_async_copy(parts[p], back.at[pl.ds(p * cap, cap)], sems.at[p]) for p in range(n_parts)]
    for copy in copies:
        copy.start()
    total = n_parts * cap
    ids = lax.broadcasted_iota(jnp.int32, (rows, total), 1)
    pick = [(ids == slots_ref[:, j:j + 1]).astype(jnp.float32).astype(jnp.bfloat16) for j in range(2)]
    for copy in copies:
        copy.wait()
    for c in range(width // COL_CHUNK):
        cols = pl.ds(c * COL_CHUNK, COL_CHUNK)
        mixed = sum(gates_ref[:, j:j + 1] * jnp.dot(pick[j], back[:, cols], preferred_element_type=jnp.float32) for j in range(2))
        y_ref[:, cols] = (x_ref[:, cols].astype(jnp.float32) + mixed).astype(jnp.bfloat16)
    if with_norm:
        def y_of(c):
            return y_ref[:, pl.ds(c * COL_CHUNK, COL_CHUNK)].astype(jnp.float32)

        norm_and_gates(y_of, h_ref, next_gates_ref, norm_ref, router_ref, routes_ref, rows, width)


def combine(x, gates, slots, parts, next_args):
    rows, width = x.shape
    cap, n = parts[0].shape[0], len(parts)
    out_shape = [jax.ShapeDtypeStruct((rows, width), jnp.bfloat16)]
    if next_args:
        out_shape += [jax.ShapeDtypeStruct((rows, width), jnp.bfloat16), jax.ShapeDtypeStruct((rows, 2), jnp.float32)]
    return pl.pallas_call(
        functools.partial(combine_kernel, bool(next_args), n),
        out_shape=tuple(out_shape),
        in_specs=[VMEM] * 3 + [ANY] * n + [VMEM] * len(next_args), out_specs=tuple([VMEM] * len(out_shape)),
        scratch_shapes=[pltpu.VMEM((n * cap, width), jnp.bfloat16), pltpu.SemaphoreType.DMA((n,))],
        compiler_params=pltpu.CompilerParams(vmem_limit_bytes=VMEM_BYTES),
        cost_estimate=pl.CostEstimate(flops=12_000_000_000, bytes_accessed=(n * cap + 3 * rows) * width * 2, transcendentals=0),
        name="combine",
    )(x, gates, slots, *parts, *next_args)


def dot_nt(rows, weight_t):
    return lax.dot_general(rows, weight_t, (((1,), (1,)), ((), ())), preferred_element_type=jnp.float32)


def ffn_kernel(layer, local, n_blocks, *refs):
    half_ref, ranks_ref = refs[:2]
    h_refs = refs[2:2 + n_blocks]
    own_g, own_u, own_d, mate_g, mate_u, mate_d = refs[2 + n_blocks:8 + n_blocks]
    far = refs[8 + n_blocks:16 + n_blocks]
    outs = refs[16 + n_blocks:16 + 2 * n_blocks]
    wg, wu, wd, picked, act, sem_g, sem_u, sem_d = refs[16 + 2 * n_blocks:]
    cap = outs[0].shape[0]
    width = wg.shape[2]
    half = width // 2
    first = half_ref[0]
    lo = pl.multiple_of(first * half, half)
    hi = pl.multiple_of((1 - first) * half, half)

    for f, (g, u, d) in enumerate(((own_g, own_u, own_d), (mate_g, mate_u, mate_d))):
        pltpu.make_async_copy(g.at[layer, local], wg.at[f], sem_g.at[f]).start()
        pltpu.make_async_copy(u.at[layer, local], wu.at[f], sem_u.at[f]).start()
    for f, (a_gu, b_gu, a_d, b_d) in ((2, far[:4]), (3, far[4:])):
        for gu, start in ((a_gu, lo), (b_gu, hi)):
            pltpu.make_async_copy(gu.at[0], wg.at[f, :, pl.ds(start, half)], sem_g.at[f]).start()
            pltpu.make_async_copy(gu.at[1], wu.at[f, :, pl.ds(start, half)], sem_u.at[f]).start()
    for f, d in enumerate((own_d, mate_d)):
        pltpu.make_async_copy(d.at[layer, local], wd.at[f], sem_d.at[f]).start()
    for f, (a_gu, b_gu, a_d, b_d) in ((2, far[:4]), (3, far[4:])):
        for d, start in ((a_d, lo), (b_d, hi)):
            pltpu.make_async_copy(d, wd.at[f, :, pl.ds(start, half)], sem_d.at[f]).start()

    for b in range(n_blocks):
        slot = lax.broadcasted_iota(jnp.int32, (cap, ranks_ref.shape[1]), 0)
        pick = (slot == ranks_ref[b:b + 1, :]).astype(jnp.float32).astype(jnp.bfloat16)

        def pick_cols(c, _, b=b, pick=pick):
            cols = pl.ds(pl.multiple_of(c * COL_CHUNK, COL_CHUNK), COL_CHUNK)
            picked[pl.ds(b * cap, cap), cols] = jnp.dot(pick, h_refs[b][:, cols], preferred_element_type=jnp.float32).astype(jnp.bfloat16)
            return _

        lax.fori_loop(0, width // COL_CHUNK, pick_cols, 0)

    def up_step(f, _):
        pltpu.make_async_copy(wg.at[f], wg.at[f], sem_g.at[f]).wait()
        pltpu.make_async_copy(wu.at[f], wu.at[f], sem_u.at[f]).wait()
        pre_gate = dot_nt(picked[...], wg[f])
        pre_up = dot_nt(picked[...], wu[f])
        act[f] = (jax.nn.silu(pre_gate) * pre_up).astype(jnp.bfloat16)
        return _

    lax.fori_loop(0, 4, up_step, 0)
    for f in range(4):
        pltpu.make_async_copy(wd.at[f], wd.at[f], sem_d.at[f]).wait()

    def down_step(c, _):
        cols = pl.ds(pl.multiple_of(c * COL_CHUNK, COL_CHUNK), COL_CHUNK)
        total = jnp.dot(act[0], wd[0, :, cols], preferred_element_type=jnp.float32)
        for f in range(1, 4):
            total += jnp.dot(act[f], wd[f, :, cols], preferred_element_type=jnp.float32)
        for b in range(n_blocks):
            outs[b][:, cols] = total[b * cap:(b + 1) * cap].astype(jnp.bfloat16)
        return _

    lax.fori_loop(0, width // COL_CHUNK, down_step, 0)


def ffn(layer, local, cap, half_idx, ranks, blocks, own, mate, far):
    n = len(blocks)
    width = blocks[0].shape[1]
    ff = own[0].shape[2]
    rows = n * cap
    return pl.pallas_call(
        functools.partial(ffn_kernel, layer, local, n),
        out_shape=tuple([jax.ShapeDtypeStruct((cap, width), jnp.bfloat16)] * n),
        in_specs=[SMEM, VMEM] + [VMEM] * n + [ANY] * 14, out_specs=tuple([VMEM] * n),
        scratch_shapes=[pltpu.VMEM((4, ff, width), jnp.bfloat16), pltpu.VMEM((4, ff, width), jnp.bfloat16),
                        pltpu.VMEM((4, ff, width), jnp.bfloat16), pltpu.VMEM((rows, width), jnp.bfloat16),
                        pltpu.VMEM((4, rows, ff), jnp.bfloat16), pltpu.SemaphoreType.DMA((4,)),
                        pltpu.SemaphoreType.DMA((4,)), pltpu.SemaphoreType.DMA((4,))],
        compiler_params=pltpu.CompilerParams(vmem_limit_bytes=VMEM_BYTES),
        cost_estimate=pl.CostEstimate(flops=6 * rows * width * 4 * ff, bytes_accessed=12 * width * ff * 2 + 4 * rows * width * 2, transcendentals=0),
        name="expert_ffn",
    )(half_idx, ranks, *blocks, *own, *mate, *far)


def solution(mesh):
    n_ep, n_fs, n_rep = mesh.shape["ep"], mesh.shape["fsdp"], mesh.shape["rep"]
    token_spec = P(("rep", "ep", "fsdp"), None)
    expert_in_spec = P(None, "ep", None, "fsdp")
    expert_out_spec = P(None, "ep", "fsdp", None)
    route_spec = P(None, ("rep", "ep", "fsdp"), None)
    to_mate = [(f, f ^ 1) for f in range(n_fs)]
    to_far = [(f, f ^ 2) for f in range(n_fs)]
    to_rep = [(r, r ^ 1) for r in range(n_rep)]

    def device_step(x_in, norm_w, router_w, gate_w, up_w, down_w, routes):
        layers, tok_dev, top_k = routes.shape
        n_local = gate_w.shape[1]
        width = x_in.shape[1]
        half = width // 2
        experts = router_w.shape[2]
        cap = tok_dev * top_k // 4
        rep, ep = lax.axis_index("rep"), lax.axis_index("ep")
        half_idx = rep.reshape(1).astype(jnp.int32)

        own = (gate_w.swapaxes(2, 3), up_w.swapaxes(2, 3), down_w)
        far = {}
        for l in range(layers):
            for k in range(n_local):
                g_half, u_half, d_half = (lax.dynamic_slice(t, (l, k, 0, rep * half), (1, 1, t.shape[2], half))[0, 0] for t in own)
                gu_half = jnp.stack([g_half, u_half])
                a_gu, a_d = (lax.ppermute(t, "fsdp", to_far) for t in (gu_half, d_half))
                b_gu, b_d = (lax.ppermute(t, "rep", to_rep) for t in (a_gu, a_d))
                mine = (a_gu, b_gu, a_d, b_d)
                far[l, k] = mine + tuple(lax.ppermute(t, "fsdp", to_mate) for t in mine)
        mate = tuple(lax.ppermute(t, "fsdp", to_mate) for t in own)

        all_routes = lax.all_gather(routes, "ep", axis=0)
        local_ids = ep * n_local + jnp.arange(n_local, dtype=jnp.int32)
        before = (jnp.arange(tok_dev)[:, None] < jnp.arange(tok_dev)[None, :]).astype(jnp.bfloat16)

        def rank_of(routes_blt2, ids):
            chosen = jnp.any(routes_blt2[..., None, :, :] == ids[:, None, None], axis=-1)
            rank = jnp.einsum("...t,ts->...s", chosen.astype(jnp.bfloat16), before, preferred_element_type=jnp.float32).astype(jnp.int32)
            return jnp.where(chosen, rank, -1)

        block_order = ep ^ jnp.arange(n_ep, dtype=jnp.int32)
        ranks = rank_of(all_routes[block_order], local_ids)
        own_rank = rank_of(routes, jnp.arange(experts, dtype=jnp.int32))
        pair_rank = jnp.take_along_axis(own_rank, routes.transpose(0, 2, 1), axis=1).transpose(0, 2, 1)
        slots = (((routes // n_local) ^ ep) * n_local + routes % n_local) * cap + pair_rank

        up1 = [(z, z + 1) for z in range(n_ep - 1)]
        down1 = [(z + 1, z) for z in range(n_ep - 1)]
        stream = x_in
        hidden, gates = first_norm(stream, norm_w[0:1], router_w[0], routes[0])
        for l in range(layers):
            lo1 = lax.ppermute(hidden, "ep", up1)
            hi1 = lax.ppermute(hidden, "ep", down1)
            lo2 = lax.ppermute(lo1, "ep", [(1, 2), (2, 3)])
            hi2 = lax.ppermute(hi1, "ep", [(2, 1), (1, 0)])
            lo3 = lax.ppermute(lo2, "ep", [(2, 3)])
            hi3 = lax.ppermute(hi2, "ep", [(1, 0)])
            even = ep % 2 == 0
            q1 = jnp.where(even, hi1, lo1)
            q2 = jnp.where(ep < 2, hi2, lo2)
            q3 = jnp.where(ep == 0, hi3, jnp.where(ep == 1, hi1, jnp.where(ep == 2, lo1, lo3)))
            groups = (((0, 1), (hidden, q1)), ((2,), (q2,)), ((3,), (q3,)))
            parts = {}
            for k in range(n_local):
                for qs, blocks in groups:
                    rank_rows = jnp.stack([ranks[q, l, k] for q in qs])
                    outs = ffn(l, k, cap, half_idx, rank_rows, blocks, own, mate, far[l, k])
                    for q, out in zip(qs, outs):
                        parts[q, k] = out if q == 0 else lax.ppermute(out, "ep", [(z, z ^ q) for z in range(n_ep)])
            ordered = [parts[q, k] for q in range(n_ep) for k in range(n_local)]
            if l + 1 < layers:
                stream, hidden, gates = combine(stream, gates, slots[l], ordered, (norm_w[l + 1:l + 2], router_w[l + 1], routes[l + 1]))
            else:
                stream, = combine(stream, gates, slots[l], ordered, ())
        return stream

    return jax.shard_map(device_step, mesh=mesh,
                         in_specs=(token_spec, P(), P(), expert_in_spec, expert_in_spec, expert_out_spec, route_spec),
                         out_specs=token_spec, check_vma=False)
```

```python
import functools

import jax
import jax.numpy as jnp
from jax import lax
from jax.experimental import pallas as pl
from jax.experimental.pallas import tpu as pltpu
from jax.sharding import PartitionSpec as P

NORM_EPS = 1e-5
MESH = pl.DeviceIdType.MESH
ANY = pl.BlockSpec(memory_space=pl.ANY)
VMEM = pl.BlockSpec(memory_space=pltpu.VMEM)
VMEM_BYTES = 67_043_328
MATS = 3


def dot_nt(rows, weight_t):
    return lax.dot_general(rows, weight_t, (((1,), (1,)), ((), ())), preferred_element_type=jnp.float32)


def dot(a, b):
    return jnp.dot(a, b, preferred_element_type=jnp.float32)


def layers_kernel(x_ref, norm_ref, router_ref, routes_ref, routes_row_ref, wg_ref, wu_ref, wd_ref,
                  y_ref, mate_w, far_w, mate_far_w,
                  hbuf, ranks, back, outb, picked, act, wgu, wdn, gates_ref, slots_ref,
                  ysend, yrecv, xsend, xrecv, msend, mrecv, fsend, frecv,
                  hsend, hrecv, tsend, trecv, rsend, rrecv, gu_sem, d_sem):
    n_layers, n_local, ff, width = wg_ref.shape
    tok = x_ref.shape[0]
    experts = router_ref.shape[1]
    cap = back.shape[1]
    n_ep = hbuf.shape[1]
    chunk = wdn.shape[3]
    chunks = width // chunk
    half = width // 2
    weights = (wg_ref, wu_ref, wd_ref)
    pieces = n_local * MATS
    ep = lax.axis_index("ep")
    fs = lax.axis_index("fsdp")
    rep = lax.axis_index("rep")

    def xor(i, bits):
        out = i
        for b in (1, 2):
            if bits & b:
                out = out + b - 2 * b * ((i // b) % 2)
        return out

    far_id, mate_id, rep_id = {"fsdp": xor(fs, 2)}, {"fsdp": xor(fs, 1)}, {"rep": 1 - rep}
    barrier = pltpu.get_barrier_semaphore()
    peers = [far_id, mate_id, rep_id] + [{"ep": xor(ep, q)} for q in range(1, n_ep)]
    for peer in peers:
        pl.semaphore_signal(barrier, inc=1, device_id=peer, device_id_type=MESH)
    pl.semaphore_wait(barrier, len(peers))

    def remote(src, dst, send, recv, device):
        return pltpu.make_async_remote_copy(src_ref=src, dst_ref=dst, send_sem=send, recv_sem=recv, device_id=device, device_id_type=MESH)

    mine = pl.ds(pl.multiple_of(rep * half, half), half)
    other = pl.ds(pl.multiple_of((1 - rep) * half, half), half)

    def split(i):
        return i // pieces, (i % pieces) // MATS, weights[i % MATS]

    def y_copy(i):
        l, k, w = split(i)
        return remote(w.at[l, k, :, mine], far_w.at[i, :, mine], ysend.at[i], yrecv.at[i], far_id)

    def x_copy(i):
        return remote(far_w.at[i, :, mine], far_w.at[i, :, mine], xsend.at[i], xrecv.at[i], rep_id)

    def x_arrival(i):
        return remote(far_w.at[i, :, other], far_w.at[i, :, other], xsend.at[i], xrecv.at[i], rep_id)

    def m_copy(i):
        l, k, w = split(i)
        return remote(w.at[l, k], mate_w.at[i], msend.at[i], mrecv.at[i], mate_id)

    def f_copy(i):
        return remote(far_w.at[i], mate_far_w.at[i], fsend.at[i], frecv.at[i], mate_id)

    def pass_x(i):
        y_copy(i).wait_recv()
        x_copy(i).start()

    def pass_mate(i):
        x_arrival(i).wait_recv()
        f_copy(i).start()

    def weights_ready(i):
        m_copy(i).wait_recv()
        f_copy(i).wait_recv()

    def hop_copy(l, s, up):
        block = ep - s + 1 if up else ep + s - 1
        block = jnp.clip(block, 0, n_ep - 1)
        to = jnp.clip(ep + 1 if up else ep - 1, 0, n_ep - 1)
        d = 0 if up else 1
        data = remote(hbuf.at[l, block], hbuf.at[l, block], hsend.at[l, d, s - 1], hrecv.at[l, d, s - 1], {"ep": to})
        if l:
            return (data,)
        return data, remote(ranks.at[block], ranks.at[block], tsend.at[d, s - 1], trecv.at[d, s - 1], {"ep": to})

    def sends(s, up):
        return jnp.logical_and(ep >= s - 1, ep < n_ep - 1) if up else jnp.logical_and(ep <= n_ep - s, ep > 0)

    def arrives(s, up):
        return ep >= s if up else ep < n_ep - s

    def hop_start(l, s):
        for up in (True, False):
            @pl.when(sends(s, up))
            def _(up=up):
                for copy in hop_copy(l, s, up):
                    copy.start()

    def hop_wait(l, s):
        for up in (True, False):
            @pl.when(arrives(s, up))
            def _(up=up):
                for copy in hop_copy(l, s, up):
                    copy.wait_recv()

    def hop_drain(l):
        for s in range(1, n_ep):
            for up in (True, False):
                @pl.when(sends(s, up))
                def _(s=s, up=up):
                    for copy in hop_copy(l, s, up):
                        copy.wait_send()

    def routing():
        a = lax.broadcasted_iota(jnp.int32, (tok, tok), 0)
        b = lax.broadcasted_iota(jnp.int32, (tok, tok), 1)
        upper = (a < b).astype(jnp.float32).astype(jnp.bfloat16)
        lower = (a > b).astype(jnp.float32).astype(jnp.bfloat16)
        for l in range(n_layers):
            ids = lax.broadcasted_iota(jnp.int32, (experts, tok), 0)
            chosen = jnp.logical_or(ids == routes_row_ref[l, 0:1, :], ids == routes_row_ref[l, 1:2, :])
            rank = dot(chosen.astype(jnp.float32).astype(jnp.bfloat16), upper)
            ranks[ep, pl.ds(l * experts, experts), :] = jnp.where(chosen, rank, -1.0)
            ids = lax.broadcasted_iota(jnp.int32, (tok, experts), 1)
            choice = [routes_ref[l, :, j:j + 1] for j in range(2)]
            chosen = jnp.logical_or(ids == choice[0], ids == choice[1])
            rank = dot(lower, chosen.astype(jnp.float32).astype(jnp.bfloat16))
            for j in range(2):
                pair_rank = jnp.sum(jnp.where(ids == choice[j], rank, 0.0), axis=1, keepdims=True).astype(jnp.int32)
                slots_ref[l, :, j:j + 1] = ((choice[j] // n_local) ^ ep) * (n_local * cap) + (choice[j] % n_local) * cap + pair_rank

    def norm(src_ref, l):
        h_ref = hbuf.at[l, ep]

        def cols_of(c):
            return pl.ds(pl.multiple_of(c * chunk, chunk), chunk)

        def sq_step(c, sq):
            y = src_ref[:, cols_of(c)].astype(jnp.float32)
            return sq + jnp.sum(y * y, axis=1, keepdims=True)

        inv = lax.rsqrt(lax.fori_loop(0, chunks, sq_step, jnp.zeros((tok, 1), jnp.float32)) / width + NORM_EPS)

        def h_step(c, _):
            cols = cols_of(c)
            h_ref[:, cols] = (src_ref[:, cols].astype(jnp.float32) * inv * norm_ref[l:l + 1, cols]).astype(jnp.bfloat16)
            return _

        lax.fori_loop(0, chunks, h_step, 0)

    def gates(l):
        logits = dot_nt(hbuf[l, ep], router_ref[l])
        ids = lax.broadcasted_iota(jnp.int32, logits.shape, 1)
        p = [jnp.sum(jnp.where(ids == routes_ref[l, :, j:j + 1], logits, 0.0), axis=1, keepdims=True) for j in range(2)]
        top = jnp.maximum(p[0], p[1])
        e = [jnp.exp(p[j] - top) for j in range(2)]
        for j in range(2):
            gates_ref[:, j:j + 1] = e[j] / (e[0] + e[1])

    def ffn(l, k, qs):
        base = (l * n_local + k) * MATS
        rows = len(qs) * cap

        def source(f, m):
            return (weights[m].at[l, k], mate_w.at[base + m], far_w.at[base + m], mate_far_w.at[base + m])[f]

        def gu_copies(f):
            return [pltpu.make_async_copy(source(f, m), wgu.at[f % 2, m], gu_sem.at[f % 2, m]) for m in range(2)]

        def d_copies(c, slot):
            cols = pl.ds(pl.multiple_of(c * chunk, chunk), chunk)
            return [pltpu.make_async_copy(source(f, 2).at[:, cols], wdn.at[slot, f], d_sem.at[slot, f]) for f in range(4)]

        for f in range(2):
            for copy in gu_copies(f):
                copy.start()
        for copy in d_copies(0, 0):
            copy.start()
        slot_ids = lax.broadcasted_iota(jnp.int32, (cap, tok), 0)
        for n, q in enumerate(qs):
            block = xor(ep, q)
            row = ranks[block, pl.ds(l * experts + ep * n_local + k, 1), :].astype(jnp.int32)
            pick = (slot_ids == row).astype(jnp.float32).astype(jnp.bfloat16)

            def pick_cols(c, _, n=n, block=block, pick=pick):
                cols = pl.ds(pl.multiple_of(c * chunk, chunk), chunk)
                picked[pl.ds(n * cap, cap), cols] = dot(pick, hbuf[l, block, :, cols]).astype(jnp.bfloat16)
                return _

            lax.fori_loop(0, chunks, pick_cols, 0)

        def up_step(f, _):
            slot = f % 2
            for m in range(2):
                pltpu.make_async_copy(weights[m].at[l, k], wgu.at[slot, m], gu_sem.at[slot, m]).wait()
            pre_gate = dot_nt(picked[pl.ds(0, rows), :], wgu[slot, 0])
            pre_up = dot_nt(picked[pl.ds(0, rows), :], wgu[slot, 1])
            act[f, pl.ds(0, rows), :] = (jax.nn.silu(pre_gate) * pre_up).astype(jnp.bfloat16)
            for g in range(2):
                @pl.when(f == g)
                def _(g=g):
                    for copy in gu_copies(g + 2):
                        copy.start()
            return 0

        lax.fori_loop(0, 4, up_step, 0)

        def down_step(c, _):
            slot = c % 2

            @pl.when(c + 1 < chunks)
            def _():
                for copy in d_copies(jnp.minimum(c + 1, chunks - 1), (c + 1) % 2):
                    copy.start()

            for copy in d_copies(c, slot):
                copy.wait()
            cols = pl.ds(pl.multiple_of(c * chunk, chunk), chunk)
            total = dot(act[0, pl.ds(0, rows), :], wdn[slot, 0])
            for f in range(1, 4):
                total += dot(act[f, pl.ds(0, rows), :], wdn[slot, f])
            out = total.astype(jnp.bfloat16)
            for n, q in enumerate(qs):
                piece = out[n * cap:(n + 1) * cap]
                if q == 0:
                    back[k, :, cols] = piece
                else:
                    outb[(q - 1) * n_local + k, :, cols] = piece
            return 0

        lax.fori_loop(0, chunks, down_step, 0)
        for q in qs:
            if q:
                return_copy(q, k).start()

    def return_copy(q, k):
        j = (q - 1) * n_local + k
        return remote(outb.at[j], back.at[q * n_local + k], rsend.at[j], rrecv.at[j], {"ep": xor(ep, q)})

    def combine(src_ref, l):
        for q in range(1, n_ep):
            for k in range(n_local):
                return_copy(q, k).wait_recv()
        total = n_ep * n_local * cap
        ids = lax.broadcasted_iota(jnp.int32, (tok, total), 1)
        pick = [(ids == slots_ref[l, :, j:j + 1]).astype(jnp.float32).astype(jnp.bfloat16) for j in range(2)]

        def step(c, _):
            cols = pl.ds(pl.multiple_of(c * chunk, chunk), chunk)
            rows = back[:, :, cols].reshape(total, chunk)
            mixed = gates_ref[:, 0:1] * dot(pick[0], rows) + gates_ref[:, 1:2] * dot(pick[1], rows)
            y_ref[:, cols] = (src_ref[:, cols].astype(jnp.float32) + mixed).astype(jnp.bfloat16)
            return _

        lax.fori_loop(0, chunks, step, 0)
        for q in range(1, n_ep):
            for k in range(n_local):
                return_copy(q, k).wait_send()

    for i in range(pieces):
        y_copy(i).start()
    routing()
    norm(x_ref, 0)
    hop_start(0, 1)
    for i in range(pieces):
        m_copy(i).start()
    gates(0)
    pass_x(0)
    hop_wait(0, 1)
    hop_start(0, 2)
    pass_x(1)
    pass_mate(0)
    pass_x(2)
    pass_mate(1)
    hop_wait(0, 2)
    hop_start(0, 3)
    pass_mate(2)
    pass_x(3)
    for i in range(MATS):
        weights_ready(i)
    ffn(0, 0, (2,))
    hop_wait(0, 3)
    pass_mate(3)
    ffn(0, 0, (3,))
    pass_x(4)
    pass_mate(4)
    for i in range(pieces, 2 * pieces):
        y_copy(i).start()
    ffn(0, 0, (0, 1))
    pass_x(5)
    pass_mate(5)
    for i in range(pieces, 2 * pieces):
        m_copy(i).start()
    for i in range(MATS, pieces):
        weights_ready(i)
    ffn(0, 1, (2,))
    pass_x(6)
    ffn(0, 1, (3,))
    pass_x(7)
    pass_mate(6)
    ffn(0, 1, (0, 1))
    pass_x(8)
    pass_mate(7)
    pass_x(9)
    pass_mate(8)
    combine(x_ref, 0)
    norm(y_ref, 1)
    hop_start(1, 1)
    gates(1)
    pass_x(10)
    pass_mate(9)
    pass_x(11)
    hop_wait(1, 1)
    hop_start(1, 2)
    for i in range(6, 9):
        weights_ready(i)
    ffn(1, 0, (0, 1))
    pass_mate(10)
    hop_wait(1, 2)
    hop_start(1, 3)
    ffn(1, 0, (2,))
    pass_mate(11)
    for i in range(9, 12):
        weights_ready(i)
    ffn(1, 1, (2,))
    hop_wait(1, 3)
    ffn(1, 0, (3,))
    ffn(1, 1, (3,))
    ffn(1, 1, (0, 1))
    combine(y_ref, 1)
    hop_drain(0)
    hop_drain(1)
    for i in range(2 * pieces):
        y_copy(i).wait_send()
        x_copy(i).wait_send()
        m_copy(i).wait_send()
        f_copy(i).wait_send()


def moe_layers(x, norm_w, router_t, routes, routes_row, wg, wu, wd, n_ep):
    n_layers, n_local, ff, width = wg.shape
    tok = x.shape[0]
    experts = router_t.shape[1]
    cap = tok // 2
    chunk = min(512, width // 2)
    n = n_layers * n_local * MATS
    bf = jnp.bfloat16
    dma = pltpu.SemaphoreType.DMA
    copies = jax.ShapeDtypeStruct((n, ff, width), bf)
    return pl.pallas_call(
        layers_kernel,
        out_shape=(jax.ShapeDtypeStruct((tok, width), bf), copies, copies, copies),
        in_specs=[VMEM] * 5 + [ANY] * 3, out_specs=(VMEM, ANY, ANY, ANY),
        scratch_shapes=[
            pltpu.VMEM((n_layers, n_ep, tok, width), bf), pltpu.VMEM((n_ep, n_layers * experts, tok), jnp.float32),
            pltpu.VMEM((n_ep * n_local, cap, width), bf), pltpu.VMEM(((n_ep - 1) * n_local, cap, width), bf),
            pltpu.VMEM((2 * cap, width), bf), pltpu.VMEM((4, 2 * cap, ff), bf),
            pltpu.VMEM((2, 2, ff, width), bf), pltpu.VMEM((2, 4, ff, chunk), bf),
            pltpu.VMEM((tok, 2), jnp.float32), pltpu.VMEM((n_layers, tok, 2), jnp.int32),
        ] + [dma((n,))] * 8 + [dma((n_layers, 2, n_ep - 1))] * 2 + [dma((2, n_ep - 1))] * 2
          + [dma(((n_ep - 1) * n_local,))] * 2 + [dma((2, 2)), dma((2, 4))],
        compiler_params=pltpu.CompilerParams(collective_id=0, has_side_effects=True, vmem_limit_bytes=VMEM_BYTES),
        name="moe_layers",
    )(x, norm_w, router_t, routes, routes_row, wg, wu, wd)[0]


def solution(mesh):
    token_spec = P(("rep", "ep", "fsdp"), None)
    expert_in_spec = P(None, "ep", None, "fsdp")
    expert_out_spec = P(None, "ep", "fsdp", None)
    route_spec = P(None, ("rep", "ep", "fsdp"), None)
    n_ep = mesh.shape["ep"]

    def device_step(x_in, norm_w, router_w, gate_w, up_w, down_w, routes):
        return moe_layers(x_in, norm_w, router_w.swapaxes(1, 2), routes, routes.swapaxes(1, 2),
                          gate_w.swapaxes(2, 3), up_w.swapaxes(2, 3), down_w, n_ep)

    return jax.shard_map(device_step, mesh=mesh,
                         in_specs=(token_spec, P(), P(), expert_in_spec, expert_in_spec, expert_out_spec, route_spec),
                         out_specs=token_spec, check_vma=False)
```

```python
import functools

import jax
import jax.numpy as jnp
from jax import lax
from jax.experimental import pallas as pl
from jax.experimental.pallas import tpu as pltpu
from jax.sharding import PartitionSpec as P

NORM_EPS = 1e-5
MESH = pl.DeviceIdType.MESH
ANY = pl.BlockSpec(memory_space=pl.ANY)
VMEM = pl.BlockSpec(memory_space=pltpu.VMEM)
VMEM_BYTES = 67_043_328
MATS = 3


def dot_nt(rows, weight_t):
    return lax.dot_general(rows, weight_t, (((1,), (1,)), ((), ())), preferred_element_type=jnp.float32)


def dot(a, b):
    return jnp.dot(a, b, preferred_element_type=jnp.float32)


def layers_kernel(x_ref, norm_ref, router_ref, routes_ref, routes_row_ref, wg_ref, wu_ref, wd_ref,
                  y_ref, mate_w, far_w, mate_far_w,
                  hbuf, ranks, back, outb, picked, act, wgu, wdn, acc, gates_ref, slots_ref,
                  ysend, yrecv, xsend, xrecv, msend, mrecv, fsend, frecv,
                  hsend, hrecv, tsend, trecv, rsend, rrecv, gu_sem, d_sem):
    n_layers, n_local, ff, width = wg_ref.shape
    tok = x_ref.shape[0]
    experts = router_ref.shape[1]
    cap = back.shape[1]
    n_ep = hbuf.shape[1]
    chunk = wdn.shape[3]
    chunks = width // chunk
    half = width // 2
    weights = (wg_ref, wu_ref, wd_ref)
    pieces = n_local * MATS
    ep = lax.axis_index("ep")
    fs = lax.axis_index("fsdp")
    rep = lax.axis_index("rep")

    def xor(i, bits):
        out = i
        for b in (1, 2):
            if bits & b:
                out = out + b - 2 * b * ((i // b) % 2)
        return out

    far_id, mate_id, rep_id = {"fsdp": xor(fs, 2)}, {"fsdp": xor(fs, 1)}, {"rep": 1 - rep}
    barrier = pltpu.get_barrier_semaphore()
    peers = [far_id, mate_id, rep_id] + [{"ep": xor(ep, q)} for q in range(1, n_ep)]
    for peer in peers:
        pl.semaphore_signal(barrier, inc=1, device_id=peer, device_id_type=MESH)
    pl.semaphore_wait(barrier, len(peers))

    def remote(src, dst, send, recv, device):
        return pltpu.make_async_remote_copy(src_ref=src, dst_ref=dst, send_sem=send, recv_sem=recv, device_id=device, device_id_type=MESH)

    quarter = half // 2

    def part_cols(r, s):
        return pl.ds(pl.multiple_of(r * half + s * quarter, quarter), quarter)

    def split(i):
        return i // pieces, (i % pieces) // MATS, weights[i % MATS]

    def y_copy(i, s):
        l, k, w = split(i)
        cols = part_cols(rep, s)
        return remote(w.at[l, k, :, cols], far_w.at[i, :, cols], ysend.at[i, s], yrecv.at[i, s], far_id)

    def x_copy(i, s):
        cols = part_cols(rep, s)
        return remote(far_w.at[i, :, cols], far_w.at[i, :, cols], xsend.at[i, s], xrecv.at[i, s], rep_id)

    def x_arrival(i, s):
        cols = part_cols(1 - rep, s)
        return remote(far_w.at[i, :, cols], far_w.at[i, :, cols], xsend.at[i, s], xrecv.at[i, s], rep_id)

    def m_copy(i):
        l, k, w = split(i)
        return remote(w.at[l, k], mate_w.at[i], msend.at[i], mrecv.at[i], mate_id)

    def f_copy(i):
        return remote(far_w.at[i], mate_far_w.at[i], fsend.at[i], frecv.at[i], mate_id)

    def pass_x(i, s):
        with jax.named_scope(f"pass_x#i={i}#s={s}"):
            y_copy(i, s).wait_recv()
            x_copy(i, s).start()

    def pass_mate(i):
        with jax.named_scope(f"pass_mate#i={i}"):
            for s in range(2):
                x_arrival(i, s).wait_recv()
            f_copy(i).start()

    def weights_ready(ids):
        with jax.named_scope(f"weights_ready#i={ids[0]}"):
            for i in ids:
                m_copy(i).wait_recv()
                f_copy(i).wait_recv()

    def hop_copy(l, s, up):
        block = ep - s + 1 if up else ep + s - 1
        block = jnp.clip(block, 0, n_ep - 1)
        to = jnp.clip(ep + 1 if up else ep - 1, 0, n_ep - 1)
        d = 0 if up else 1
        data = remote(hbuf.at[l, block], hbuf.at[l, block], hsend.at[l, d, s - 1], hrecv.at[l, d, s - 1], {"ep": to})
        if l:
            return (data,)
        return data, remote(ranks.at[block], ranks.at[block], tsend.at[d, s - 1], trecv.at[d, s - 1], {"ep": to})

    def sends(s, up):
        return jnp.logical_and(ep >= s - 1, ep < n_ep - 1) if up else jnp.logical_and(ep <= n_ep - s, ep > 0)

    def arrives(s, up):
        return ep >= s if up else ep < n_ep - s

    def hop_start(l, s):
        for up in (True, False):
            @pl.when(sends(s, up))
            def _(up=up):
                for copy in hop_copy(l, s, up):
                    copy.start()

    def hop_wait(l, s):
        with jax.named_scope(f"hop_wait#l={l}#s={s}"):
            for up in (True, False):
                @pl.when(arrives(s, up))
                def _(up=up):
                    for copy in hop_copy(l, s, up):
                        copy.wait_recv()

    def hop_drain(l):
        for s in range(1, n_ep):
            for up in (True, False):
                @pl.when(sends(s, up))
                def _(s=s, up=up):
                    for copy in hop_copy(l, s, up):
                        copy.wait_send()

    def routing():
        a = lax.broadcasted_iota(jnp.int32, (tok, tok), 0)
        b = lax.broadcasted_iota(jnp.int32, (tok, tok), 1)
        upper = (a < b).astype(jnp.float32).astype(jnp.bfloat16)
        lower = (a > b).astype(jnp.float32).astype(jnp.bfloat16)
        for l in range(n_layers):
            ids = lax.broadcasted_iota(jnp.int32, (experts, tok), 0)
            chosen = jnp.logical_or(ids == routes_row_ref[l, 0:1, :], ids == routes_row_ref[l, 1:2, :])
            rank = dot(chosen.astype(jnp.float32).astype(jnp.bfloat16), upper)
            ranks[ep, pl.ds(l * experts, experts), :] = jnp.where(chosen, rank, -1.0)
            ids = lax.broadcasted_iota(jnp.int32, (tok, experts), 1)
            choice = [routes_ref[l, :, j:j + 1] for j in range(2)]
            chosen = jnp.logical_or(ids == choice[0], ids == choice[1])
            rank = dot(lower, chosen.astype(jnp.float32).astype(jnp.bfloat16))
            for j in range(2):
                pair_rank = jnp.sum(jnp.where(ids == choice[j], rank, 0.0), axis=1, keepdims=True).astype(jnp.int32)
                slots_ref[l, :, j:j + 1] = ((choice[j] // n_local) ^ ep) * (n_local * cap) + (choice[j] % n_local) * cap + pair_rank

    def cols_of(c):
        return pl.ds(pl.multiple_of(c * chunk, chunk), chunk)

    def square_sum(src_ref):
        def step(c, sq):
            y = src_ref[:, cols_of(c)].astype(jnp.float32)
            return sq + jnp.sum(y * y, axis=1, keepdims=True)

        return lax.fori_loop(0, chunks, step, jnp.zeros((tok, 1), jnp.float32))

    def norm(src_ref, sq, l):
        h_ref = hbuf.at[l, ep]
        inv = lax.rsqrt(sq / width + NORM_EPS)

        def step(c, _):
            cols = cols_of(c)
            h_ref[:, cols] = (src_ref[:, cols].astype(jnp.float32) * inv * norm_ref[l:l + 1, cols]).astype(jnp.bfloat16)
            return _

        lax.fori_loop(0, chunks, step, 0)

    def gates(l):
        logits = dot_nt(hbuf[l, ep], router_ref[l])
        ids = lax.broadcasted_iota(jnp.int32, logits.shape, 1)
        p = [jnp.sum(jnp.where(ids == routes_ref[l, :, j:j + 1], logits, 0.0), axis=1, keepdims=True) for j in range(2)]
        top = jnp.maximum(p[0], p[1])
        e = [jnp.exp(p[j] - top) for j in range(2)]
        for j in range(2):
            gates_ref[:, j:j + 1] = e[j] / (e[0] + e[1])

    def source(l, k, f, m):
        i = (l * n_local + k) * MATS + m
        return (weights[m].at[l, k], mate_w.at[i], far_w.at[i], mate_far_w.at[i])[f]

    def up(l, k, q0, nq, service={}):
        with jax.named_scope(f"up#l={l}#k={k}#q={q0}"):
            span = pl.ds(q0 * cap, nq * cap)

            def gu_copies(f):
                return [pltpu.make_async_copy(source(l, k, f, m), wgu.at[f % 2, m], gu_sem.at[f % 2, m]) for m in range(2)]

            for f in range(2):
                for copy in gu_copies(f):
                    copy.start()
            slot_ids = lax.broadcasted_iota(jnp.int32, (cap, tok), 0)
            for q in range(q0, q0 + nq):
                block = xor(ep, q)
                row = ranks[block, pl.ds(l * experts + ep * n_local + k, 1), :].astype(jnp.int32)
                pick = (slot_ids == row).astype(jnp.float32).astype(jnp.bfloat16)

                def pick_cols(c, _, q=q, block=block, pick=pick):
                    cols = cols_of(c)
                    picked[pl.ds(q * cap, cap), cols] = dot(pick, hbuf[l, block, :, cols]).astype(jnp.bfloat16)
                    return _

                lax.fori_loop(0, chunks, pick_cols, 0)

            def up_step(f, _):
                slot = f % 2
                for m in range(2):
                    pltpu.make_async_copy(weights[m].at[l, k], wgu.at[slot, m], gu_sem.at[slot, m]).wait()
                pre_gate = dot_nt(picked[span, :], wgu[slot, 0])
                pre_up = dot_nt(picked[span, :], wgu[slot, 1])
                act[f, span, :] = (jax.nn.silu(pre_gate) * pre_up).astype(jnp.bfloat16)
                for g in range(4):
                    if g < 2 or g in service:
                        @pl.when(f == g)
                        def _(g=g):
                            if g < 2:
                                for copy in gu_copies(g + 2):
                                    copy.start()
                            if g in service:
                                service[g]()
                return 0

            lax.fori_loop(0, 4, up_step, 0)

    def down(l, k, q0, nq):
        with jax.named_scope(f"down#l={l}#k={k}#q={q0}"):
            span = pl.ds(q0 * cap, nq * cap)

            def d_copies(c, slot):
                return [pltpu.make_async_copy(source(l, k, f, 2).at[:, cols_of(c)], wdn.at[slot, f], d_sem.at[slot, f]) for f in range(4)]

            for copy in d_copies(0, 0):
                copy.start()

            def step(c, _):
                slot = c % 2

                @pl.when(c + 1 < chunks)
                def _():
                    for copy in d_copies(jnp.minimum(c + 1, chunks - 1), (c + 1) % 2):
                        copy.start()

                for copy in d_copies(c, slot):
                    copy.wait()
                cols = cols_of(c)
                total = dot(act[0, span, :], wdn[slot, 0])
                for f in range(1, 4):
                    total += dot(act[f, span, :], wdn[slot, f])
                out = total.astype(jnp.bfloat16)
                for n in range(nq):
                    piece = out[n * cap:(n + 1) * cap]
                    if q0 + n == 0:
                        back[k, :, cols] = piece
                    else:
                        outb[(q0 + n - 1) * n_local + k, :, cols] = piece
                return 0

            lax.fori_loop(0, chunks, step, 0)
            for q in range(q0, q0 + nq):
                if q:
                    return_copy(q, k).start()

    def return_copy(q, k):
        j = (q - 1) * n_local + k
        return remote(outb.at[j], back.at[q * n_local + k], rsend.at[j], rrecv.at[j], {"ep": xor(ep, q)})

    def add_part(l, q, k, src_ref, first=False, last=False):
        if q:
            with jax.named_scope(f"return_wait#l={l}#q={q}#k={k}"):
                return_copy(q, k).wait_recv()
        with jax.named_scope(f"add#l={l}#q={q}#k={k}"):
            j = q * n_local + k
            ids = lax.broadcasted_iota(jnp.int32, (tok, cap), 1)
            at = [slots_ref[l, :, c:c + 1] - j * cap for c in range(2)]
            pick = jnp.logical_or(ids == at[0], ids == at[1]).astype(jnp.float32).astype(jnp.bfloat16)
            gate = sum(jnp.where(jnp.logical_and(at[c] >= 0, at[c] < cap), gates_ref[:, c:c + 1], 0.0) for c in range(2))

            def step(c, sq):
                cols = cols_of(c)
                before = src_ref[:, cols].astype(jnp.float32) if first else acc[:, cols]
                after = before + gate * dot(pick, back[j, :, cols])
                if not last:
                    acc[:, cols] = after
                    return sq
                y = after.astype(jnp.bfloat16)
                y_ref[:, cols] = y
                y = y.astype(jnp.float32)
                return sq + jnp.sum(y * y, axis=1, keepdims=True)

            return lax.fori_loop(0, chunks, step, jnp.zeros((tok, 1), jnp.float32))

    def returns_sent():
        for q in range(1, n_ep):
            for k in range(n_local):
                return_copy(q, k).wait_send()

    inner = jnp.logical_and(ep > 0, ep < n_ep - 1)
    outer = jnp.logical_not(inner)
    for i in range(pieces):
        for s in range(2):
            y_copy(i, s).start()
    with jax.named_scope("routing"):
        routing()
    with jax.named_scope("norm0"):
        norm(x_ref, square_sum(x_ref), 0)
    hop_start(0, 1)
    for i in range(pieces):
        m_copy(i).start()
    gates(0)
    pass_x(0, 0)
    pass_x(0, 1)
    pass_x(1, 0)
    pass_mate(0)
    hop_wait(0, 1)
    hop_start(0, 2)
    pass_x(1, 1)
    pass_x(2, 0)
    pass_mate(1)
    weights_ready((0, 1))
    up(0, 0, 0, 2, {1: lambda: pass_x(2, 1)})
    hop_wait(0, 2)
    hop_start(0, 3)
    pass_x(3, 0)
    up(0, 0, 2, 1, {1: lambda: pass_mate(2), 3: lambda: pass_x(3, 1)})
    weights_ready((2,))
    down(0, 0, 2, 1)
    for i in range(pieces, 2 * pieces):
        for s in range(2):
            y_copy(i, s).start()
    down(0, 0, 0, 2)
    pass_x(4, 0)
    pass_mate(3)
    hop_wait(0, 3)
    up(0, 0, 3, 1, {1: lambda: pass_x(4, 1)})
    down(0, 0, 3, 1)
    pass_x(5, 0)
    pass_mate(4)
    weights_ready((3, 4))
    up(0, 1, 0, 4, {1: lambda: pass_x(5, 1), 3: lambda: pass_mate(5)})
    weights_ready((5,))
    down(0, 1, 2, 1)
    pass_x(6, 0)
    down(0, 1, 3, 1)
    down(0, 1, 0, 2)
    pass_x(6, 1)
    for i in range(pieces, 2 * pieces):
        m_copy(i).start()
    add_part(0, 0, 0, x_ref, first=True)
    pass_x(7, 0)
    pass_mate(6)
    add_part(0, 0, 1, x_ref)
    add_part(0, 1, 0, x_ref)
    add_part(0, 2, 0, x_ref)
    pass_x(7, 1)
    add_part(0, 3, 0, x_ref)
    pass_x(8, 0)
    pass_mate(7)
    add_part(0, 1, 1, x_ref)
    add_part(0, 2, 1, x_ref)
    pass_x(8, 1)
    pass_x(9, 0)
    pass_mate(8)
    square = add_part(0, 3, 1, x_ref, last=True)
    norm(y_ref, square, 1)
    hop_start(1, 1)
    pass_x(9, 1)
    returns_sent()
    gates(1)
    pass_x(10, 0)
    pass_mate(9)
    pass_x(10, 1)
    pass_x(11, 0)
    pass_mate(10)
    hop_wait(1, 1)
    hop_start(1, 2)
    weights_ready((6, 7))

    @pl.when(inner)
    def _():
        up(1, 0, 3, 1)
        up(1, 0, 0, 2)

    @pl.when(outer)
    def _():
        up(1, 0, 0, 2)

    pass_x(11, 1)
    weights_ready((8,))

    @pl.when(inner)
    def _():
        down(1, 0, 3, 1)

    down(1, 0, 0, 2)
    hop_wait(1, 2)
    hop_start(1, 3)
    pass_mate(11)
    up(1, 0, 2, 1)
    down(1, 0, 2, 1)
    weights_ready((9, 10))
    up(1, 1, 0, 3)
    weights_ready((11,))
    down(1, 1, 2, 1)

    @pl.when(inner)
    def _():
        up(1, 1, 3, 1)

    @pl.when(outer)
    def _():
        hop_wait(1, 3)
        up(1, 0, 3, 1)
        down(1, 0, 3, 1)
        up(1, 1, 3, 1)

    down(1, 1, 3, 1)
    down(1, 1, 0, 2)
    add_part(1, 0, 0, y_ref, first=True)
    add_part(1, 0, 1, y_ref)
    add_part(1, 1, 0, y_ref)
    add_part(1, 2, 0, y_ref)
    add_part(1, 1, 1, y_ref)
    add_part(1, 2, 1, y_ref)
    add_part(1, 3, 0, y_ref)
    add_part(1, 3, 1, y_ref, last=True)
    returns_sent()
    hop_drain(0)
    hop_drain(1)
    for i in range(2 * pieces):
        for s in range(2):
            y_copy(i, s).wait_send()
            x_copy(i, s).wait_send()
        m_copy(i).wait_send()
        f_copy(i).wait_send()


def moe_layers(x, norm_w, router_t, routes, routes_row, wg, wu, wd, n_ep):
    n_layers, n_local, ff, width = wg.shape
    tok = x.shape[0]
    experts = router_t.shape[1]
    cap = tok // 2
    chunk = min(512, width // 2)
    n = n_layers * n_local * MATS
    bf = jnp.bfloat16
    dma = pltpu.SemaphoreType.DMA
    copies = jax.ShapeDtypeStruct((n, ff, width), bf)
    return pl.pallas_call(
        layers_kernel,
        out_shape=(jax.ShapeDtypeStruct((tok, width), bf), copies, copies, copies),
        in_specs=[VMEM] * 5 + [ANY] * 3, out_specs=(VMEM, ANY, ANY, ANY),
        scratch_shapes=[
            pltpu.VMEM((n_layers, n_ep, tok, width), bf), pltpu.VMEM((n_ep, n_layers * experts, tok), jnp.float32),
            pltpu.VMEM((n_ep * n_local, cap, width), bf), pltpu.VMEM(((n_ep - 1) * n_local, cap, width), bf),
            pltpu.VMEM((n_ep * cap, width), bf), pltpu.VMEM((4, n_ep * cap, ff), bf),
            pltpu.VMEM((2, 2, ff, width), bf), pltpu.VMEM((2, 4, ff, chunk), bf),
            pltpu.VMEM((tok, width), jnp.float32),
            pltpu.VMEM((tok, 2), jnp.float32), pltpu.VMEM((n_layers, tok, 2), jnp.int32),
        ] + [dma((n, 2))] * 4 + [dma((n,))] * 4 + [dma((n_layers, 2, n_ep - 1))] * 2 + [dma((2, n_ep - 1))] * 2
          + [dma(((n_ep - 1) * n_local,))] * 2 + [dma((2, 2)), dma((2, 4))],
        compiler_params=pltpu.CompilerParams(collective_id=0, has_side_effects=True, vmem_limit_bytes=VMEM_BYTES),
        name="moe_layers",
    )(x, norm_w, router_t, routes, routes_row, wg, wu, wd)[0]


def solution(mesh):
    token_spec = P(("rep", "ep", "fsdp"), None)
    expert_in_spec = P(None, "ep", None, "fsdp")
    expert_out_spec = P(None, "ep", "fsdp", None)
    route_spec = P(None, ("rep", "ep", "fsdp"), None)
    n_ep = mesh.shape["ep"]

    def device_step(x_in, norm_w, router_w, gate_w, up_w, down_w, routes):
        return moe_layers(x_in, norm_w, router_w.swapaxes(1, 2), routes, routes.swapaxes(1, 2),
                          gate_w.swapaxes(2, 3), up_w.swapaxes(2, 3), down_w, n_ep)

    return jax.shard_map(device_step, mesh=mesh,
                         in_specs=(token_spec, P(), P(), expert_in_spec, expert_in_spec, expert_out_spec, route_spec),
                         out_specs=token_spec, check_vma=False)
```

```python
import functools

import jax
import jax.numpy as jnp
from jax import lax
from jax.experimental import pallas as pl
from jax.experimental.pallas import tpu as pltpu
from jax.sharding import PartitionSpec as P

NORM_EPS = 1e-5
MESH = pl.DeviceIdType.MESH
ANY = pl.BlockSpec(memory_space=pl.ANY)
VMEM = pl.BlockSpec(memory_space=pltpu.VMEM)
VMEM_BYTES = 67_043_328
MATS = 3


def dot_nt(rows, weight_t):
    return lax.dot_general(rows, weight_t, (((1,), (1,)), ((), ())), preferred_element_type=jnp.float32)


def dot(a, b):
    return jnp.dot(a, b, preferred_element_type=jnp.float32)


def layers_kernel(x_ref, norm_ref, router_ref, routes_ref, routes_row_ref, wg_ref, wu_ref, wd_ref,
                  y_ref, mate_w, far_w, mate_far_w,
                  hbuf, ranks, back, outb, picked, act, wgu, wdn, acc, gates_ref, slots_ref,
                  ysend, yrecv, xsend, xrecv, msend, mrecv, fsend, frecv,
                  hsend, hrecv, tsend, trecv, rsend, rrecv, gu_sem, d_sem, xs_ref, x_sem):
    n_layers, n_local, ff, width = wg_ref.shape
    tok = x_ref.shape[0]
    experts = router_ref.shape[1]
    cap = back.shape[1]
    n_ep = hbuf.shape[1]
    chunk = wdn.shape[3]
    chunks = width // chunk
    half = width // 2
    weights = (wg_ref, wu_ref, wd_ref)
    pieces = n_local * MATS
    ep = lax.axis_index("ep")
    fs = lax.axis_index("fsdp")
    rep = lax.axis_index("rep")

    def xor(i, bits):
        out = i
        for b in (1, 2):
            if bits & b:
                out = out + b - 2 * b * ((i // b) % 2)
        return out

    far_id, mate_id, rep_id = {"fsdp": xor(fs, 2)}, {"fsdp": xor(fs, 1)}, {"rep": 1 - rep}
    barrier = pltpu.get_barrier_semaphore()
    peers = [far_id, mate_id, rep_id] + [{"ep": xor(ep, q)} for q in range(1, n_ep)]
    for peer in peers:
        pl.semaphore_signal(barrier, inc=1, device_id=peer, device_id_type=MESH)
    pl.semaphore_wait(barrier, len(peers))

    def remote(src, dst, send, recv, device):
        return pltpu.make_async_remote_copy(src_ref=src, dst_ref=dst, send_sem=send, recv_sem=recv, device_id=device, device_id_type=MESH)

    def subs(i):
        return range(4 if i < pieces else 2)

    def part_cols(r, i, s):
        size = half // len(subs(i))
        return pl.ds(pl.multiple_of(r * half + s * size, size), size)

    def split(i):
        return i // pieces, (i % pieces) // MATS, weights[i % MATS]

    def y_copy(i, s):
        l, k, w = split(i)
        cols = part_cols(rep, i, s)
        return remote(w.at[l, k, :, cols], far_w.at[i, :, cols], ysend.at[i, s], yrecv.at[i, s], far_id)

    def x_copy(i, s):
        cols = part_cols(rep, i, s)
        return remote(far_w.at[i, :, cols], far_w.at[i, :, cols], xsend.at[i, s], xrecv.at[i, s], rep_id)

    def x_arrival(i, s):
        cols = part_cols(1 - rep, i, s)
        return remote(far_w.at[i, :, cols], far_w.at[i, :, cols], xsend.at[i, s], xrecv.at[i, s], rep_id)

    def m_copy(i):
        l, k, w = split(i)
        return remote(w.at[l, k], mate_w.at[i], msend.at[i], mrecv.at[i], mate_id)

    def f_copy(i, s, crossed):
        cols = part_cols(1 - rep if crossed else rep, i, s)
        c = int(crossed)
        return remote(far_w.at[i, :, cols], mate_far_w.at[i, :, cols], fsend.at[i, s, c], frecv.at[i, s, c], mate_id)

    waiting_y = [(16.0 + 7.55 * (i * 4 + s + 1) if i < pieces else 16.0 + 7.55 * (4 * pieces + 2 * ((i - pieces) * 2 + s + 1)), i, s)
                 for i in range(2 * pieces) for s in subs(i)]
    waiting_x = []
    x_free = [0.0]

    def pass_x(now):
        _, i, s = waiting_y.pop(0)
        with jax.named_scope(f"pass_x#i={i}#s={s}"):
            y_copy(i, s).wait_recv()
            x_copy(i, s).start()
            f_copy(i, s, False).start()
        x_free[0] = max(now, x_free[0]) + (7.55 if i < pieces else 15.1)
        waiting_x.append((x_free[0] + 1.0, i, s))

    def pass_mate():
        _, i, s = waiting_x.pop(0)
        with jax.named_scope(f"pass_mate#i={i}#s={s}"):
            x_arrival(i, s).wait_recv()
            f_copy(i, s, True).start()

    def serve(now, mates=True):
        while True:
            if waiting_y and waiting_y[0][0] <= now:
                pass_x(now)
            elif mates and waiting_x and waiting_x[0][0] <= now:
                pass_mate()
            else:
                return

    def serve_until(i):
        while (waiting_y and waiting_y[0][1] <= i) or (waiting_x and waiting_x[0][1] <= i):
            if waiting_y and (not waiting_x or waiting_y[0][0] <= waiting_x[0][0]):
                pass_x(waiting_y[0][0])
            else:
                pass_mate()

    def weights_ready(ids):
        serve_until(ids[-1])
        with jax.named_scope(f"weights_ready#i={ids[0]}"):
            for i in ids:
                m_copy(i).wait_recv()
                for s in subs(i):
                    for crossed in (False, True):
                        f_copy(i, s, crossed).wait_recv()

    def hop_copy(l, s, up):
        block = ep - s + 1 if up else ep + s - 1
        block = jnp.clip(block, 0, n_ep - 1)
        to = jnp.clip(ep + 1 if up else ep - 1, 0, n_ep - 1)
        d = 0 if up else 1
        data = remote(hbuf.at[l, block], hbuf.at[l, block], hsend.at[l, d, s - 1], hrecv.at[l, d, s - 1], {"ep": to})
        if l:
            return (data,)
        return data, remote(ranks.at[block], ranks.at[block], tsend.at[d, s - 1], trecv.at[d, s - 1], {"ep": to})

    def sends(s, up):
        return jnp.logical_and(ep >= s - 1, ep < n_ep - 1) if up else jnp.logical_and(ep <= n_ep - s, ep > 0)

    def arrives(s, up):
        return ep >= s if up else ep < n_ep - s

    def hop_start(l, s):
        for up in (True, False):
            @pl.when(sends(s, up))
            def _(up=up):
                for copy in hop_copy(l, s, up):
                    copy.start()

    def hop_wait(l, s):
        with jax.named_scope(f"hop_wait#l={l}#s={s}"):
            for up in (True, False):
                @pl.when(arrives(s, up))
                def _(up=up):
                    for copy in hop_copy(l, s, up):
                        copy.wait_recv()

    def hop_drain(l):
        for s in range(1, n_ep):
            for up in (True, False):
                @pl.when(sends(s, up))
                def _(s=s, up=up):
                    for copy in hop_copy(l, s, up):
                        copy.wait_send()

    def routing():
        a = lax.broadcasted_iota(jnp.int32, (tok, tok), 0)
        b = lax.broadcasted_iota(jnp.int32, (tok, tok), 1)
        upper = (a < b).astype(jnp.float32).astype(jnp.bfloat16)
        lower = (a > b).astype(jnp.float32).astype(jnp.bfloat16)
        for l in range(n_layers):
            ids = lax.broadcasted_iota(jnp.int32, (experts, tok), 0)
            chosen = jnp.logical_or(ids == routes_row_ref[l, 0:1, :], ids == routes_row_ref[l, 1:2, :])
            rank = dot(chosen.astype(jnp.float32).astype(jnp.bfloat16), upper)
            ranks[ep, pl.ds(l * experts, experts), :] = jnp.where(chosen, rank, -1.0)
            ids = lax.broadcasted_iota(jnp.int32, (tok, experts), 1)
            choice = [routes_ref[l, :, j:j + 1] for j in range(2)]
            chosen = jnp.logical_or(ids == choice[0], ids == choice[1])
            rank = dot(lower, chosen.astype(jnp.float32).astype(jnp.bfloat16))
            for j in range(2):
                pair_rank = jnp.sum(jnp.where(ids == choice[j], rank, 0.0), axis=1, keepdims=True).astype(jnp.int32)
                slots_ref[l, :, j:j + 1] = ((choice[j] // n_local) ^ ep) * (n_local * cap) + (choice[j] % n_local) * cap + pair_rank

    def cols_of(c):
        return pl.ds(pl.multiple_of(c * chunk, chunk), chunk)

    def square_sum(src_ref):
        def step(c, sq):
            y = src_ref[:, cols_of(c)].astype(jnp.float32)
            return sq + jnp.sum(y * y, axis=1, keepdims=True)

        return lax.fori_loop(0, chunks, step, jnp.zeros((tok, 1), jnp.float32))

    def norm(src_ref, sq, l):
        h_ref = hbuf.at[l, ep]
        inv = lax.rsqrt(sq / width + NORM_EPS)

        def step(c, _):
            cols = cols_of(c)
            h_ref[:, cols] = (src_ref[:, cols].astype(jnp.float32) * inv * norm_ref[l:l + 1, cols]).astype(jnp.bfloat16)
            return _

        lax.fori_loop(0, chunks, step, 0)

    def gates(l):
        logits = dot_nt(hbuf[l, ep], router_ref[l])
        ids = lax.broadcasted_iota(jnp.int32, logits.shape, 1)
        p = [jnp.sum(jnp.where(ids == routes_ref[l, :, j:j + 1], logits, 0.0), axis=1, keepdims=True) for j in range(2)]
        top = jnp.maximum(p[0], p[1])
        e = [jnp.exp(p[j] - top) for j in range(2)]
        for j in range(2):
            gates_ref[:, j:j + 1] = e[j] / (e[0] + e[1])

    place = (0, 1, 3, 2)
    def source(l, k, f, m):
        i = (l * n_local + k) * MATS + m
        return (weights[m].at[l, k], mate_w.at[i], far_w.at[i], mate_far_w.at[i])[f]

    def up(l, k, qs, service={}):
        with jax.named_scope(f"up#l={l}#k={k if isinstance(k, int) else 2}#q={qs[0]}#n={len(qs)}"):
            span = pl.ds(place[qs[0]] * cap, len(qs) * cap)

            def gu_copies(f):
                return [pltpu.make_async_copy(source(l, k, f, m), wgu.at[f % 2, m], gu_sem.at[f % 2, m]) for m in range(2)]

            for f in range(2):
                for copy in gu_copies(f):
                    copy.start()
            slot_ids = lax.broadcasted_iota(jnp.int32, (cap, tok), 0)
            for q in qs:
                block = xor(ep, q)
                row = ranks[block, pl.ds(l * experts + ep * n_local + k, 1), :].astype(jnp.int32)
                pick = (slot_ids == row).astype(jnp.float32).astype(jnp.bfloat16)

                def pick_cols(c, _, q=q, block=block, pick=pick):
                    cols = cols_of(c)
                    picked[pl.ds(place[q] * cap, cap), cols] = dot(pick, hbuf[l, block, :, cols]).astype(jnp.bfloat16)
                    return _

                lax.fori_loop(0, chunks, pick_cols, 0)

            def up_step(f, _):
                slot = f % 2
                for m in range(2):
                    pltpu.make_async_copy(weights[m].at[l, k], wgu.at[slot, m], gu_sem.at[slot, m]).wait()
                pre_gate = dot_nt(picked[span, :], wgu[slot, 0])
                pre_up = dot_nt(picked[span, :], wgu[slot, 1])
                act[f, span, :] = (jax.nn.silu(pre_gate) * pre_up).astype(jnp.bfloat16)
                for g in range(4):
                    if g < 2 or g in service:
                        @pl.when(f == g)
                        def _(g=g):
                            if g < 2:
                                for copy in gu_copies(g + 2):
                                    copy.start()
                            if g in service:
                                service[g]()
                return 0

            lax.fori_loop(0, 4, up_step, 0)

    def down(l, k, qs):
        with jax.named_scope(f"down#l={l}#k={k if isinstance(k, int) else 2}#q={qs[0]}"):
            span = pl.ds(place[qs[0]] * cap, len(qs) * cap)

            def d_copies(c, slot):
                return [pltpu.make_async_copy(source(l, k, f, 2).at[:, cols_of(c)], wdn.at[slot, f], d_sem.at[slot, f]) for f in range(4)]

            for copy in d_copies(0, 0):
                copy.start()

            def step(c, _):
                slot = c % 2

                @pl.when(c + 1 < chunks)
                def _():
                    for copy in d_copies(jnp.minimum(c + 1, chunks - 1), (c + 1) % 2):
                        copy.start()

                for copy in d_copies(c, slot):
                    copy.wait()
                cols = cols_of(c)
                total = dot(act[0, span, :], wdn[slot, 0])
                for f in range(1, 4):
                    total += dot(act[f, span, :], wdn[slot, f])
                out = total.astype(jnp.bfloat16)
                for n, q in enumerate(qs):
                    piece = out[n * cap:(n + 1) * cap]
                    if q == 0:
                        back[k, :, cols] = piece
                    else:
                        outb[(q - 1) * n_local + k, :, cols] = piece
                return 0

            lax.fori_loop(0, chunks, step, 0)
            for q in qs:
                if q:
                    return_copy(q, k).start()

    def return_copy(q, k):
        j = (q - 1) * n_local + k
        return remote(outb.at[j], back.at[q * n_local + k], rsend.at[j], rrecv.at[j], {"ep": xor(ep, q)})

    def start_sum(src_ref):
        def step(c, _):
            acc[:, cols_of(c)] = src_ref[:, cols_of(c)].astype(jnp.float32)
            return 0

        lax.fori_loop(0, chunks, step, 0)

    def part(l, j):
        ids = lax.broadcasted_iota(jnp.int32, (tok, cap), 1)
        at = [slots_ref[l, :, c:c + 1] - j * cap for c in range(2)]
        pick = jnp.logical_or(ids == at[0], ids == at[1]).astype(jnp.float32).astype(jnp.bfloat16)
        gate = sum(jnp.where(jnp.logical_and(at[c] >= 0, at[c] < cap), gates_ref[:, c:c + 1], 0.0) for c in range(2))
        return pick, gate

    def landed(j):
        r = j - n_local
        remote(outb.at[r], back.at[j], rsend.at[r], rrecv.at[r], {"ep": ep}).wait_recv()

    def add_parts(l, first, stride, count):
        def body(n, _):
            j = first + stride * n
            with jax.named_scope(f"add#l={l}#j={first}"):
                if first >= n_local:
                    landed(j)
                elif first + stride * count > n_local:
                    @pl.when(j >= n_local)
                    def _():
                        landed(jnp.maximum(j, n_local))
                pick, gate = part(l, j)

                def step(c, _):
                    cols = cols_of(c)
                    acc[:, cols] += gate * dot(pick, back[j, :, cols])
                    return 0

                lax.fori_loop(0, chunks, step, 0)
            return 0

        lax.fori_loop(0, count, body, 0)

    def add_last(l):
        j = n_ep * n_local - 1
        with jax.named_scope(f"return_wait#l={l}"):
            landed(j)
        with jax.named_scope(f"add_last#l={l}"):
            pick, gate = part(l, j)

            def step(c, sq):
                cols = cols_of(c)
                y = (acc[:, cols] + gate * dot(pick, back[j, :, cols])).astype(jnp.bfloat16)
                y_ref[:, cols] = y
                y = y.astype(jnp.float32)
                return sq + jnp.sum(y * y, axis=1, keepdims=True)

            return lax.fori_loop(0, chunks, step, jnp.zeros((tok, 1), jnp.float32))

    def returns_sent():
        for q in range(1, n_ep):
            for k in range(n_local):
                return_copy(q, k).wait_send()

    inner = jnp.logical_and(ep > 0, ep < n_ep - 1)
    outer = jnp.logical_not(inner)
    x_load = pltpu.make_async_copy(x_ref, xs_ref, x_sem)
    x_load.start()
    for i in range(pieces):
        for s in subs(i):
            y_copy(i, s).start()
    with jax.named_scope("routing"):
        routing()
    x_load.wait()
    with jax.named_scope("norm0"):
        norm(xs_ref, square_sum(xs_ref), 0)
    hop_start(0, 1)
    for i in range(pieces):
        m_copy(i).start()
    gates(0)
    serve(59.0)
    hop_wait(0, 1)
    hop_start(0, 2)
    weights_ready((0, 1))

    @pl.when(inner)
    def _():
        up(0, 0, (0, 1, 3))

    @pl.when(outer)
    def _():
        up(0, 0, (0, 1))

    serve(108.0)
    hop_wait(0, 2)
    hop_start(0, 3)
    for i in range(pieces, 2 * pieces):
        for s in subs(i):
            y_copy(i, s).start()
    up(0, 0, (2,), {0: lambda: serve(115.0), 2: lambda: serve(119.0)})
    weights_ready((2,))

    @pl.when(inner)
    def _():
        down(0, 0, (3,))

    serve(131.0)
    down(0, 0, (2,))
    serve(139.0)
    down(0, 0, (0, 1))
    serve(157.0)
    hop_wait(0, 3)

    @pl.when(outer)
    def _():
        up(0, 0, (3,))

    serve(166.0)

    @pl.when(outer)
    def _():
        down(0, 0, (3,))

    weights_ready((3, 4))
    up(0, 1, (0, 1, 3, 2), {0: lambda: serve(188.0), 1: lambda: serve(192.0), 2: lambda: serve(197.0), 3: lambda: serve(201.0)})
    weights_ready((5,))
    down(0, 1, (3,))
    serve(219.0)
    down(0, 1, (2,))
    serve(227.0)
    down(0, 1, (0, 1))
    for i in range(pieces, 2 * pieces):
        m_copy(i).start()
    serve(236.0)
    start_sum(xs_ref)
    add_parts(0, 0, 1, n_local)
    serve(243.0)
    add_parts(0, 2, 2, 3)
    serve(290.0)
    add_parts(0, 3, 2, 2)
    serve(305.0, mates=False)
    square = add_last(0)
    norm(y_ref, square, 1)
    hop_start(1, 1)
    returns_sent()
    gates(1)
    serve(360.0)
    hop_wait(1, 1)
    hop_start(1, 2)
    weights_ready((6, 7))

    @pl.when(inner)
    def _():
        up(1, 0, (0, 1, 3))

    @pl.when(outer)
    def _():
        up(1, 0, (0, 1))

    serve(383.0)
    weights_ready((8,))

    @pl.when(inner)
    def _():
        down(1, 0, (3,))

    @pl.when(outer)
    def _():
        down(1, 0, (0, 1))

    weights_ready((9, 10))

    @pl.when(inner)
    def _():
        up(1, 1, (3,))

    @pl.when(outer)
    def _():
        up(1, 1, (0, 1))

    hop_wait(1, 2)
    hop_start(1, 3)
    weights_ready((11,))

    @pl.when(inner)
    def _():
        down(1, 1, (3,))

    @pl.when(outer)
    def _():
        down(1, 1, (0, 1))

    def both(qs):
        def body(k, _):
            up(1, k, qs)
            down(1, k, qs)
            return 0

        lax.fori_loop(0, n_local, body, 0)

    both((2,))

    @pl.when(inner)
    def _():
        down(1, 0, (0, 1))
        up(1, 1, (0, 1))
        down(1, 1, (0, 1))

    @pl.when(outer)
    def _():
        hop_wait(1, 3)
        both((3,))

    start_sum(y_ref)
    add_parts(1, 0, 1, n_ep * n_local - 1)
    add_last(1)
    returns_sent()
    hop_drain(0)
    hop_drain(1)
    for i in range(2 * pieces):
        for s in subs(i):
            y_copy(i, s).wait_send()
            x_copy(i, s).wait_send()
            for crossed in (False, True):
                f_copy(i, s, crossed).wait_send()
        m_copy(i).wait_send()


def moe_layers(x, norm_w, router_t, routes, routes_row, wg, wu, wd, n_ep):
    n_layers, n_local, ff, width = wg.shape
    tok = x.shape[0]
    experts = router_t.shape[1]
    cap = tok // 2
    chunk = min(512, width // 2)
    n = n_layers * n_local * MATS
    bf = jnp.bfloat16
    dma = pltpu.SemaphoreType.DMA
    copies = jax.ShapeDtypeStruct((n, ff, width), bf)
    return pl.pallas_call(
        layers_kernel,
        out_shape=(jax.ShapeDtypeStruct((tok, width), bf), copies, copies, copies),
        in_specs=[ANY] + [VMEM] * 4 + [ANY] * 3, out_specs=(VMEM, ANY, ANY, ANY),
        scratch_shapes=[
            pltpu.VMEM((n_layers, n_ep, tok, width), bf), pltpu.VMEM((n_ep, n_layers * experts, tok), jnp.float32),
            pltpu.VMEM((n_ep * n_local, cap, width), bf), pltpu.VMEM(((n_ep - 1) * n_local, cap, width), bf),
            pltpu.VMEM((n_ep * cap, width), bf), pltpu.VMEM((4, n_ep * cap, ff), bf),
            pltpu.VMEM((2, 2, ff, width), bf), pltpu.VMEM((2, 4, ff, chunk), bf),
            pltpu.VMEM((tok, width), jnp.float32),
            pltpu.VMEM((tok, 2), jnp.float32), pltpu.VMEM((n_layers, tok, 2), jnp.int32),
        ] + [dma((n, 4))] * 4 + [dma((n,))] * 2 + [dma((n, 4, 2))] * 2 + [dma((n_layers, 2, n_ep - 1))] * 2 + [dma((2, n_ep - 1))] * 2
          + [dma(((n_ep - 1) * n_local,))] * 2 + [dma((2, 2)), dma((2, 4)), pltpu.VMEM((tok, width), bf), dma],
        compiler_params=pltpu.CompilerParams(collective_id=0, has_side_effects=True, vmem_limit_bytes=VMEM_BYTES),
        name="moe_layers",
    )(x, norm_w, router_t, routes, routes_row, wg, wu, wd)[0]


def solution(mesh):
    token_spec = P(("rep", "ep", "fsdp"), None)
    expert_in_spec = P(None, "ep", None, "fsdp")
    expert_out_spec = P(None, "ep", "fsdp", None)
    route_spec = P(None, ("rep", "ep", "fsdp"), None)
    n_ep = mesh.shape["ep"]

    def device_step(x_in, norm_w, router_w, gate_w, up_w, down_w, routes):
        return moe_layers(x_in, norm_w, router_w.swapaxes(1, 2), routes, routes.swapaxes(1, 2),
                          gate_w.swapaxes(2, 3), up_w.swapaxes(2, 3), down_w, n_ep)

    return jax.shard_map(device_step, mesh=mesh,
                         in_specs=(token_spec, P(), P(), expert_in_spec, expert_in_spec, expert_out_spec, route_spec),
                         out_specs=token_spec, check_vma=False)
```

```python
import functools

import jax
import jax.numpy as jnp
from jax import lax
from jax.experimental import pallas as pl
from jax.experimental.pallas import tpu as pltpu
from jax.sharding import PartitionSpec as P

NORM_EPS = 1e-5
MESH = pl.DeviceIdType.MESH
ANY = pl.BlockSpec(memory_space=pl.ANY)
VMEM = pl.BlockSpec(memory_space=pltpu.VMEM)
VMEM_BYTES = 67_043_328
MATS = 3


def dot_nt(rows, weight_t):
    return lax.dot_general(rows, weight_t, (((1,), (1,)), ((), ())), preferred_element_type=jnp.float32)


def dot(a, b):
    return jnp.dot(a, b, preferred_element_type=jnp.float32)


def layers_kernel(x_ref, norm_ref, router_ref, routes_ref, routes_row_ref, wg_ref, wu_ref, wd_ref,
                  y_ref, mate_w, far_w, mate_far_w,
                  hbuf, ranks, back, outb, picked, act, wgu, wdn, acc, gates_ref, slots_ref,
                  ysend, yrecv, xsend, xrecv, msend, mrecv, fsend, frecv,
                  hsend, hrecv, tsend, trecv, rsend, rrecv, gu_sem, d_sem, xs_ref, x_sem):
    n_layers, n_local, ff, width = wg_ref.shape
    tok = x_ref.shape[0]
    experts = router_ref.shape[1]
    cap = back.shape[1]
    n_ep = hbuf.shape[1]
    chunk = wdn.shape[3]
    chunks = width // chunk
    half = width // 2
    weights = (wg_ref, wu_ref, wd_ref)
    pieces = n_local * MATS
    ep = lax.axis_index("ep")
    fs = lax.axis_index("fsdp")
    rep = lax.axis_index("rep")

    def xor(i, bits):
        out = i
        for b in (1, 2):
            if bits & b:
                out = out + b - 2 * b * ((i // b) % 2)
        return out

    far_id, mate_id, rep_id = {"fsdp": xor(fs, 2)}, {"fsdp": xor(fs, 1)}, {"rep": 1 - rep}
    barrier = pltpu.get_barrier_semaphore()
    peers = [far_id, mate_id, rep_id] + [{"ep": xor(ep, q)} for q in range(1, n_ep)]
    for peer in peers:
        pl.semaphore_signal(barrier, inc=1, device_id=peer, device_id_type=MESH)
    pl.semaphore_wait(barrier, len(peers))

    def remote(src, dst, send, recv, device):
        return pltpu.make_async_remote_copy(src_ref=src, dst_ref=dst, send_sem=send, recv_sem=recv, device_id=device, device_id_type=MESH)

    def subs(i):
        return range(4 if i < pieces else 2)

    def part_cols(r, i, s):
        size = half // len(subs(i))
        return pl.ds(pl.multiple_of(r * half + s * size, size), size)

    def split(i):
        return i // pieces, (i % pieces) // MATS, weights[i % MATS]

    def y_copy(i, s):
        l, k, w = split(i)
        cols = part_cols(rep, i, s)
        return remote(w.at[l, k, :, cols], far_w.at[i, :, cols], ysend.at[i, s], yrecv.at[i, s], far_id)

    def x_copy(i, s):
        cols = part_cols(rep, i, s)
        return remote(far_w.at[i, :, cols], far_w.at[i, :, cols], xsend.at[i, s], xrecv.at[i, s], rep_id)

    def x_arrival(i, s):
        cols = part_cols(1 - rep, i, s)
        return remote(far_w.at[i, :, cols], far_w.at[i, :, cols], xsend.at[i, s], xrecv.at[i, s], rep_id)

    def m_copy(i):
        l, k, w = split(i)
        return remote(w.at[l, k], mate_w.at[i], msend.at[i], mrecv.at[i], mate_id)

    def f_copy(i, s, crossed):
        cols = part_cols(1 - rep if crossed else rep, i, s)
        c = int(crossed)
        return remote(far_w.at[i, :, cols], mate_far_w.at[i, :, cols], fsend.at[i, s, c], frecv.at[i, s, c], mate_id)

    waiting_y = [(16.0 + 7.55 * (i * 4 + s + 1) if i < pieces else 16.0 + 7.55 * (4 * pieces + 2 * ((i - pieces) * 2 + s + 1)), i, s)
                 for i in range(2 * pieces) for s in subs(i)]
    waiting_x = []
    x_free = [0.0]

    def pass_x():
        landed_at, i, s = waiting_y.pop(0)
        with jax.named_scope(f"pass_x#i={i}#s={s}"):
            y_copy(i, s).wait_recv()
            x_copy(i, s).start()
            f_copy(i, s, False).start()
        x_free[0] = max(landed_at, x_free[0]) + (7.55 if i < pieces else 15.1)
        waiting_x.append((x_free[0] + 1.0, i, s))

    def pass_mate():
        _, i, s = waiting_x.pop(0)
        with jax.named_scope(f"pass_mate#i={i}#s={s}"):
            x_arrival(i, s).wait_recv()
            f_copy(i, s, True).start()

    def serve(now, mates=True):
        while True:
            if waiting_y and waiting_y[0][0] <= now:
                pass_x()
            elif mates and waiting_x and waiting_x[0][0] <= now:
                pass_mate()
            else:
                return

    def serve_until(i):
        while (waiting_y and waiting_y[0][1] <= i) or (waiting_x and waiting_x[0][1] <= i):
            if waiting_y and (not waiting_x or waiting_y[0][0] <= waiting_x[0][0]):
                pass_x()
            else:
                pass_mate()

    def weights_ready(ids):
        serve_until(ids[-1])
        with jax.named_scope(f"weights_ready#i={ids[0]}"):
            for i in ids:
                m_copy(i).wait_recv()
                for s in subs(i):
                    for crossed in (False, True):
                        f_copy(i, s, crossed).wait_recv()

    def hop_copy(l, s, up):
        block = ep - s + 1 if up else ep + s - 1
        block = jnp.clip(block, 0, n_ep - 1)
        to = jnp.clip(ep + 1 if up else ep - 1, 0, n_ep - 1)
        d = 0 if up else 1
        data = remote(hbuf.at[l, block], hbuf.at[l, block], hsend.at[l, d, s - 1], hrecv.at[l, d, s - 1], {"ep": to})
        if l:
            return (data,)
        return data, remote(ranks.at[block], ranks.at[block], tsend.at[d, s - 1], trecv.at[d, s - 1], {"ep": to})

    def sends(s, up):
        return jnp.logical_and(ep >= s - 1, ep < n_ep - 1) if up else jnp.logical_and(ep <= n_ep - s, ep > 0)

    def arrives(s, up):
        return ep >= s if up else ep < n_ep - s

    def hop_start(l, s):
        for up in (True, False):
            @pl.when(sends(s, up))
            def _(up=up):
                for copy in hop_copy(l, s, up):
                    copy.start()

    def hop_wait(l, s):
        with jax.named_scope(f"hop_wait#l={l}#s={s}"):
            for up in (True, False):
                @pl.when(arrives(s, up))
                def _(up=up):
                    for copy in hop_copy(l, s, up):
                        copy.wait_recv()

    def hop_drain(l):
        for s in range(1, n_ep):
            for up in (True, False):
                @pl.when(sends(s, up))
                def _(s=s, up=up):
                    for copy in hop_copy(l, s, up):
                        copy.wait_send()

    def routing():
        a = lax.broadcasted_iota(jnp.int32, (tok, tok), 0)
        b = lax.broadcasted_iota(jnp.int32, (tok, tok), 1)
        upper = (a < b).astype(jnp.float32).astype(jnp.bfloat16)
        lower = (a > b).astype(jnp.float32).astype(jnp.bfloat16)
        for l in range(n_layers):
            ids = lax.broadcasted_iota(jnp.int32, (experts, tok), 0)
            chosen = jnp.logical_or(ids == routes_row_ref[l, 0:1, :], ids == routes_row_ref[l, 1:2, :])
            rank = dot(chosen.astype(jnp.float32).astype(jnp.bfloat16), upper)
            ranks[ep, pl.ds(l * experts, experts), :] = jnp.where(chosen, rank, -1.0)
            ids = lax.broadcasted_iota(jnp.int32, (tok, experts), 1)
            choice = [routes_ref[l, :, j:j + 1] for j in range(2)]
            chosen = jnp.logical_or(ids == choice[0], ids == choice[1])
            rank = dot(lower, chosen.astype(jnp.float32).astype(jnp.bfloat16))
            for j in range(2):
                pair_rank = jnp.sum(jnp.where(ids == choice[j], rank, 0.0), axis=1, keepdims=True).astype(jnp.int32)
                slots_ref[l, :, j:j + 1] = ((choice[j] // n_local) ^ ep) * (n_local * cap) + (choice[j] % n_local) * cap + pair_rank

    def cols_of(c):
        return pl.ds(pl.multiple_of(c * chunk, chunk), chunk)

    def square_sum(src_ref):
        def step(c, sq):
            y = src_ref[:, cols_of(c)].astype(jnp.float32)
            return sq + jnp.sum(y * y, axis=1, keepdims=True)

        return lax.fori_loop(0, chunks, step, jnp.zeros((tok, 1), jnp.float32))

    def norm(src_ref, sq, l):
        h_ref = hbuf.at[l, ep]
        inv = lax.rsqrt(sq / width + NORM_EPS)

        def step(c, _):
            cols = cols_of(c)
            h_ref[:, cols] = (src_ref[:, cols].astype(jnp.float32) * inv * norm_ref[l:l + 1, cols]).astype(jnp.bfloat16)
            return _

        lax.fori_loop(0, chunks, step, 0)

    def gates(l):
        logits = dot_nt(hbuf[l, ep], router_ref[l])
        ids = lax.broadcasted_iota(jnp.int32, logits.shape, 1)
        p = [jnp.sum(jnp.where(ids == routes_ref[l, :, j:j + 1], logits, 0.0), axis=1, keepdims=True) for j in range(2)]
        top = jnp.maximum(p[0], p[1])
        e = [jnp.exp(p[j] - top) for j in range(2)]
        for j in range(2):
            gates_ref[:, j:j + 1] = e[j] / (e[0] + e[1])

    place = (0, 1, 3, 2)
    def source(l, k, f, m):
        i = (l * n_local + k) * MATS + m
        return (weights[m].at[l, k], mate_w.at[i], far_w.at[i], mate_far_w.at[i])[f]

    def up(l, k, qs, service={}):
        with jax.named_scope(f"up#l={l}#k={k if isinstance(k, int) else 2}#q={qs[0]}#n={len(qs)}"):
            span = pl.ds(place[qs[0]] * cap, len(qs) * cap)

            def gu_copies(f):
                return [pltpu.make_async_copy(source(l, k, f, m), wgu.at[f % 2, m], gu_sem.at[f % 2, m]) for m in range(2)]

            for f in range(2):
                for copy in gu_copies(f):
                    copy.start()
            slot_ids = lax.broadcasted_iota(jnp.int32, (cap, tok), 0)
            for q in qs:
                block = xor(ep, q)
                row = ranks[block, pl.ds(l * experts + ep * n_local + k, 1), :].astype(jnp.int32)
                pick = (slot_ids == row).astype(jnp.float32).astype(jnp.bfloat16)

                def pick_cols(c, _, q=q, block=block, pick=pick):
                    cols = cols_of(c)
                    picked[pl.ds(place[q] * cap, cap), cols] = dot(pick, hbuf[l, block, :, cols]).astype(jnp.bfloat16)
                    return _

                lax.fori_loop(0, chunks, pick_cols, 0)

            def up_step(f, _):
                slot = f % 2
                for m in range(2):
                    pltpu.make_async_copy(weights[m].at[l, k], wgu.at[slot, m], gu_sem.at[slot, m]).wait()
                pre_gate = dot_nt(picked[span, :], wgu[slot, 0])
                pre_up = dot_nt(picked[span, :], wgu[slot, 1])
                act[f, span, :] = (jax.nn.silu(pre_gate) * pre_up).astype(jnp.bfloat16)
                for g in range(4):
                    if g < 2 or g in service:
                        @pl.when(f == g)
                        def _(g=g):
                            if g < 2:
                                for copy in gu_copies(g + 2):
                                    copy.start()
                            if g in service:
                                service[g]()
                return 0

            lax.fori_loop(0, 4, up_step, 0)

    def down(l, k, qs):
        with jax.named_scope(f"down#l={l}#k={k if isinstance(k, int) else 2}#q={qs[0]}"):
            span = pl.ds(place[qs[0]] * cap, len(qs) * cap)

            def d_copies(c, slot):
                return [pltpu.make_async_copy(source(l, k, f, 2).at[:, cols_of(c)], wdn.at[slot, f], d_sem.at[slot, f]) for f in range(4)]

            for copy in d_copies(0, 0):
                copy.start()

            def step(c, _):
                slot = c % 2

                @pl.when(c + 1 < chunks)
                def _():
                    for copy in d_copies(jnp.minimum(c + 1, chunks - 1), (c + 1) % 2):
                        copy.start()

                for copy in d_copies(c, slot):
                    copy.wait()
                cols = cols_of(c)
                total = dot(act[0, span, :], wdn[slot, 0])
                for f in range(1, 4):
                    total += dot(act[f, span, :], wdn[slot, f])
                out = total.astype(jnp.bfloat16)
                for n, q in enumerate(qs):
                    piece = out[n * cap:(n + 1) * cap]
                    if q == 0:
                        back[k, :, cols] = piece
                    else:
                        outb[(q - 1) * n_local + k, :, cols] = piece
                return 0

            lax.fori_loop(0, chunks, step, 0)
            for q in qs:
                if q:
                    return_copy(q, k).start()

    def return_copy(q, k):
        j = (q - 1) * n_local + k
        return remote(outb.at[j], back.at[q * n_local + k], rsend.at[j], rrecv.at[j], {"ep": xor(ep, q)})

    def start_sum(src_ref):
        def step(c, _):
            acc[:, cols_of(c)] = src_ref[:, cols_of(c)].astype(jnp.float32)
            return 0

        lax.fori_loop(0, chunks, step, 0)

    def part(l, j):
        ids = lax.broadcasted_iota(jnp.int32, (tok, cap), 1)
        at = [slots_ref[l, :, c:c + 1] - j * cap for c in range(2)]
        pick = jnp.logical_or(ids == at[0], ids == at[1]).astype(jnp.float32).astype(jnp.bfloat16)
        gate = sum(jnp.where(jnp.logical_and(at[c] >= 0, at[c] < cap), gates_ref[:, c:c + 1], 0.0) for c in range(2))
        return pick, gate

    def landed(j):
        r = j - n_local
        remote(outb.at[r], back.at[j], rsend.at[r], rrecv.at[r], {"ep": ep}).wait_recv()

    def add_parts(l, first, stride, count):
        def body(n, _):
            j = first + stride * n
            with jax.named_scope(f"add#l={l}#j={first}"):
                if first >= n_local:
                    landed(j)
                elif first + stride * count > n_local:
                    @pl.when(j >= n_local)
                    def _():
                        landed(jnp.maximum(j, n_local))
                pick, gate = part(l, j)

                def step(c, _):
                    cols = cols_of(c)
                    acc[:, cols] += gate * dot(pick, back[j, :, cols])
                    return 0

                lax.fori_loop(0, chunks, step, 0)
            return 0

        lax.fori_loop(0, count, body, 0)

    def add_last(l):
        j = n_ep * n_local - 1
        with jax.named_scope(f"return_wait#l={l}"):
            landed(j)
        with jax.named_scope(f"add_last#l={l}"):
            pick, gate = part(l, j)

            def step(c, sq):
                cols = cols_of(c)
                y = (acc[:, cols] + gate * dot(pick, back[j, :, cols])).astype(jnp.bfloat16)
                y_ref[:, cols] = y
                y = y.astype(jnp.float32)
                return sq + jnp.sum(y * y, axis=1, keepdims=True)

            return lax.fori_loop(0, chunks, step, jnp.zeros((tok, 1), jnp.float32))

    def returns_sent():
        for q in range(1, n_ep):
            for k in range(n_local):
                return_copy(q, k).wait_send()

    inner = jnp.logical_and(ep > 0, ep < n_ep - 1)
    outer = jnp.logical_not(inner)
    x_load = pltpu.make_async_copy(x_ref, xs_ref, x_sem)
    x_load.start()
    for i in range(pieces):
        for s in subs(i):
            y_copy(i, s).start()
    with jax.named_scope("routing"):
        routing()
    x_load.wait()
    with jax.named_scope("norm0"):
        norm(xs_ref, square_sum(xs_ref), 0)
    hop_start(0, 1)
    for i in range(pieces):
        m_copy(i).start()
    gates(0)
    serve(59.0)
    hop_wait(0, 1)
    hop_start(0, 2)
    weights_ready((0, 1))

    up(0, 0, (0, 1), {1: lambda: serve(94.0), 3: lambda: serve(101.5)})

    @pl.when(inner)
    def _():
        up(0, 0, (3,))

    serve(109.0)
    hop_wait(0, 2)
    hop_start(0, 3)
    for i in range(pieces, 2 * pieces):
        for s in subs(i):
            y_copy(i, s).start()
    up(0, 0, (2,), {0: lambda: serve(115.0), 2: lambda: serve(119.0)})
    weights_ready((2,))

    @pl.when(inner)
    def _():
        down(0, 0, (3,))

    serve(131.0)
    down(0, 0, (2,))
    serve(139.0)
    down(0, 0, (0, 1))
    serve(154.0)
    hop_wait(0, 3)

    @pl.when(outer)
    def _():
        up(0, 0, (3,))

    serve(166.0)

    @pl.when(outer)
    def _():
        down(0, 0, (3,))

    weights_ready((3, 4))
    up(0, 1, (0, 1, 3, 2), {0: lambda: serve(188.0), 1: lambda: serve(192.0), 2: lambda: serve(197.0), 3: lambda: serve(201.0)})
    weights_ready((5,))
    down(0, 1, (3,))
    serve(219.0)
    down(0, 1, (2,))
    serve(227.0)
    down(0, 1, (0, 1))
    for i in range(pieces, 2 * pieces):
        m_copy(i).start()
    serve(236.0)
    start_sum(xs_ref)
    add_parts(0, 0, 1, n_local)
    serve(243.0)
    add_parts(0, 2, 2, 3)
    serve(290.0)
    add_parts(0, 3, 2, 2)
    serve(305.0, mates=False)
    square = add_last(0)
    norm(y_ref, square, 1)
    hop_start(1, 1)
    returns_sent()
    gates(1)
    serve(360.0)
    hop_wait(1, 1)
    hop_start(1, 2)
    weights_ready((6, 7))

    @pl.when(inner)
    def _():
        up(1, 0, (0, 1, 3))

    @pl.when(outer)
    def _():
        up(1, 0, (0, 1))

    serve(383.0)
    weights_ready((8,))

    @pl.when(inner)
    def _():
        down(1, 0, (3,))

    @pl.when(outer)
    def _():
        down(1, 0, (0, 1))

    weights_ready((9, 10))

    @pl.when(inner)
    def _():
        up(1, 1, (3,))

    @pl.when(outer)
    def _():
        up(1, 1, (0, 1))

    hop_wait(1, 2)
    hop_start(1, 3)
    weights_ready((11,))

    @pl.when(inner)
    def _():
        down(1, 1, (3,))
        down(1, 0, (0, 1))

    @pl.when(outer)
    def _():
        down(1, 1, (0, 1))

    def both(qs):
        def body(k, _):
            up(1, k, qs)
            down(1, k, qs)
            return 0

        lax.fori_loop(0, n_local, body, 0)

    both((2,))

    @pl.when(inner)
    def _():
        up(1, 1, (0, 1))
        down(1, 1, (0, 1))

    @pl.when(outer)
    def _():
        hop_wait(1, 3)
        both((3,))

    start_sum(y_ref)
    add_parts(1, 0, 1, n_ep * n_local - 1)
    add_last(1)
    returns_sent()
    hop_drain(0)
    hop_drain(1)
    for i in range(2 * pieces):
        for s in subs(i):
            y_copy(i, s).wait_send()
            x_copy(i, s).wait_send()
            for crossed in (False, True):
                f_copy(i, s, crossed).wait_send()
        m_copy(i).wait_send()


def moe_layers(x, norm_w, router_t, routes, routes_row, wg, wu, wd, n_ep):
    n_layers, n_local, ff, width = wg.shape
    tok = x.shape[0]
    experts = router_t.shape[1]
    cap = tok // 2
    chunk = min(512, width // 2)
    n = n_layers * n_local * MATS
    bf = jnp.bfloat16
    dma = pltpu.SemaphoreType.DMA
    copies = jax.ShapeDtypeStruct((n, ff, width), bf)
    return pl.pallas_call(
        layers_kernel,
        out_shape=(jax.ShapeDtypeStruct((tok, width), bf), copies, copies, copies),
        in_specs=[ANY] + [VMEM] * 4 + [ANY] * 3, out_specs=(VMEM, ANY, ANY, ANY),
        scratch_shapes=[
            pltpu.VMEM((n_layers, n_ep, tok, width), bf), pltpu.VMEM((n_ep, n_layers * experts, tok), jnp.float32),
            pltpu.VMEM((n_ep * n_local, cap, width), bf), pltpu.VMEM(((n_ep - 1) * n_local, cap, width), bf),
            pltpu.VMEM((n_ep * cap, width), bf), pltpu.VMEM((4, n_ep * cap, ff), bf),
            pltpu.VMEM((2, 2, ff, width), bf), pltpu.VMEM((2, 4, ff, chunk), bf),
            pltpu.VMEM((tok, width), jnp.float32),
            pltpu.VMEM((tok, 2), jnp.float32), pltpu.VMEM((n_layers, tok, 2), jnp.int32),
        ] + [dma((n, 4))] * 4 + [dma((n,))] * 2 + [dma((n, 4, 2))] * 2 + [dma((n_layers, 2, n_ep - 1))] * 2 + [dma((2, n_ep - 1))] * 2
          + [dma(((n_ep - 1) * n_local,))] * 2 + [dma((2, 2)), dma((2, 4)), pltpu.VMEM((tok, width), bf), dma],
        compiler_params=pltpu.CompilerParams(collective_id=0, has_side_effects=True, vmem_limit_bytes=VMEM_BYTES),
        name="moe_layers",
    )(x, norm_w, router_t, routes, routes_row, wg, wu, wd)[0]


def solution(mesh):
    token_spec = P(("rep", "ep", "fsdp"), None)
    expert_in_spec = P(None, "ep", None, "fsdp")
    expert_out_spec = P(None, "ep", "fsdp", None)
    route_spec = P(None, ("rep", "ep", "fsdp"), None)
    n_ep = mesh.shape["ep"]

    def device_step(x_in, norm_w, router_w, gate_w, up_w, down_w, routes):
        return moe_layers(x_in, norm_w, router_w.swapaxes(1, 2), routes, routes.swapaxes(1, 2),
                          gate_w.swapaxes(2, 3), up_w.swapaxes(2, 3), down_w, n_ep)

    return jax.shard_map(device_step, mesh=mesh,
                         in_specs=(token_spec, P(), P(), expert_in_spec, expert_in_spec, expert_out_spec, route_spec),
                         out_specs=token_spec, check_vma=False)
```

```python
import functools

import jax
import jax.numpy as jnp
from jax import lax
from jax.experimental import pallas as pl
from jax.experimental.pallas import tpu as pltpu
from jax.sharding import PartitionSpec as P

NORM_EPS = 1e-5
MESH = pl.DeviceIdType.MESH
ANY = pl.BlockSpec(memory_space=pl.ANY)
VMEM = pl.BlockSpec(memory_space=pltpu.VMEM)
VMEM_BYTES = 67_043_328
MATS = 3


def dot_nt(rows, weight_t):
    return lax.dot_general(rows, weight_t, (((1,), (1,)), ((), ())), preferred_element_type=jnp.float32)


def dot(a, b):
    return jnp.dot(a, b, preferred_element_type=jnp.float32)


def layers_kernel(x_ref, norm_ref, router_ref, routes_ref, routes_row_ref, wg_ref, wu_ref, wd_ref,
                  y_ref, mate_w, far_w, mate_far_w,
                  hbuf, ranks, back, outb, picked, act, wgu, wdn, acc, gates_ref, slots_ref,
                  ysend, yrecv, xsend, xrecv, msend, mrecv, fsend, frecv,
                  hsend, hrecv, tsend, trecv, rsend, rrecv, gu_sem, d_sem):
    n_layers, n_local, ff, width = wg_ref.shape
    tok = x_ref.shape[0]
    experts = router_ref.shape[1]
    cap = back.shape[1]
    n_ep = hbuf.shape[1]
    chunk = wdn.shape[3]
    chunks = width // chunk
    half = width // 2
    weights = (wg_ref, wu_ref, wd_ref)
    pieces = n_local * MATS
    ep = lax.axis_index("ep")
    fs = lax.axis_index("fsdp")
    rep = lax.axis_index("rep")

    def xor(i, bits):
        out = i
        for b in (1, 2):
            if bits & b:
                out = out + b - 2 * b * ((i // b) % 2)
        return out

    far_id, mate_id, rep_id = {"fsdp": xor(fs, 2)}, {"fsdp": xor(fs, 1)}, {"rep": 1 - rep}
    barrier = pltpu.get_barrier_semaphore()
    peers = [far_id, mate_id, rep_id] + [{"ep": xor(ep, q)} for q in range(1, n_ep)]
    for peer in peers:
        pl.semaphore_signal(barrier, inc=1, device_id=peer, device_id_type=MESH)
    pl.semaphore_wait(barrier, len(peers))

    def remote(src, dst, send, recv, device):
        return pltpu.make_async_remote_copy(src_ref=src, dst_ref=dst, send_sem=send, recv_sem=recv, device_id=device, device_id_type=MESH)

    quarter = half // 2

    def part_cols(r, s):
        return pl.ds(pl.multiple_of(r * half + s * quarter, quarter), quarter)

    def split(i):
        return i // pieces, (i % pieces) // MATS, weights[i % MATS]

    def y_copy(i, s):
        l, k, w = split(i)
        cols = part_cols(rep, s)
        return remote(w.at[l, k, :, cols], far_w.at[i, :, cols], ysend.at[i, s], yrecv.at[i, s], far_id)

    def x_copy(i, s):
        cols = part_cols(rep, s)
        return remote(far_w.at[i, :, cols], far_w.at[i, :, cols], xsend.at[i, s], xrecv.at[i, s], rep_id)

    def x_arrival(i, s):
        cols = part_cols(1 - rep, s)
        return remote(far_w.at[i, :, cols], far_w.at[i, :, cols], xsend.at[i, s], xrecv.at[i, s], rep_id)

    def m_copy(i):
        l, k, w = split(i)
        return remote(w.at[l, k], mate_w.at[i], msend.at[i], mrecv.at[i], mate_id)

    def f_copy(i):
        return remote(far_w.at[i], mate_far_w.at[i], fsend.at[i], frecv.at[i], mate_id)

    def pass_x(i, s):
        with jax.named_scope(f"pass_x#i={i}#s={s}"):
            y_copy(i, s).wait_recv()
            x_copy(i, s).start()

    def pass_mate(i):
        with jax.named_scope(f"pass_mate#i={i}"):
            for s in range(2):
                x_arrival(i, s).wait_recv()
            f_copy(i).start()

    def weights_ready(ids):
        with jax.named_scope(f"weights_ready#i={ids[0]}"):
            for i in ids:
                m_copy(i).wait_recv()
                f_copy(i).wait_recv()

    def hop_copy(l, s, up):
        block = ep - s + 1 if up else ep + s - 1
        block = jnp.clip(block, 0, n_ep - 1)
        to = jnp.clip(ep + 1 if up else ep - 1, 0, n_ep - 1)
        d = 0 if up else 1
        data = remote(hbuf.at[l, block], hbuf.at[l, block], hsend.at[l, d, s - 1], hrecv.at[l, d, s - 1], {"ep": to})
        if l:
            return (data,)
        return data, remote(ranks.at[block], ranks.at[block], tsend.at[d, s - 1], trecv.at[d, s - 1], {"ep": to})

    def sends(s, up):
        return jnp.logical_and(ep >= s - 1, ep < n_ep - 1) if up else jnp.logical_and(ep <= n_ep - s, ep > 0)

    def arrives(s, up):
        return ep >= s if up else ep < n_ep - s

    def hop_start(l, s):
        for up in (True, False):
            @pl.when(sends(s, up))
            def _(up=up):
                for copy in hop_copy(l, s, up):
                    copy.start()

    def hop_wait(l, s):
        with jax.named_scope(f"hop_wait#l={l}#s={s}"):
            for up in (True, False):
                @pl.when(arrives(s, up))
                def _(up=up):
                    for copy in hop_copy(l, s, up):
                        copy.wait_recv()

    def hop_drain(l):
        for s in range(1, n_ep):
            for up in (True, False):
                @pl.when(sends(s, up))
                def _(s=s, up=up):
                    for copy in hop_copy(l, s, up):
                        copy.wait_send()

    def routing():
        a = lax.broadcasted_iota(jnp.int32, (tok, tok), 0)
        b = lax.broadcasted_iota(jnp.int32, (tok, tok), 1)
        upper = (a < b).astype(jnp.float32).astype(jnp.bfloat16)
        lower = (a > b).astype(jnp.float32).astype(jnp.bfloat16)
        for l in range(n_layers):
            ids = lax.broadcasted_iota(jnp.int32, (experts, tok), 0)
            chosen = jnp.logical_or(ids == routes_row_ref[l, 0:1, :], ids == routes_row_ref[l, 1:2, :])
            rank = dot(chosen.astype(jnp.float32).astype(jnp.bfloat16), upper)
            ranks[ep, pl.ds(l * experts, experts), :] = jnp.where(chosen, rank, -1.0)
            ids = lax.broadcasted_iota(jnp.int32, (tok, experts), 1)
            choice = [routes_ref[l, :, j:j + 1] for j in range(2)]
            chosen = jnp.logical_or(ids == choice[0], ids == choice[1])
            rank = dot(lower, chosen.astype(jnp.float32).astype(jnp.bfloat16))
            for j in range(2):
                pair_rank = jnp.sum(jnp.where(ids == choice[j], rank, 0.0), axis=1, keepdims=True).astype(jnp.int32)
                slots_ref[l, :, j:j + 1] = ((choice[j] // n_local) ^ ep) * (n_local * cap) + (choice[j] % n_local) * cap + pair_rank

    def cols_of(c):
        return pl.ds(pl.multiple_of(c * chunk, chunk), chunk)

    def square_sum(src_ref):
        def step(c, sq):
            y = src_ref[:, cols_of(c)].astype(jnp.float32)
            return sq + jnp.sum(y * y, axis=1, keepdims=True)

        return lax.fori_loop(0, chunks, step, jnp.zeros((tok, 1), jnp.float32))

    def norm(src_ref, sq, l):
        h_ref = hbuf.at[l, ep]
        inv = lax.rsqrt(sq / width + NORM_EPS)

        def step(c, _):
            cols = cols_of(c)
            h_ref[:, cols] = (src_ref[:, cols].astype(jnp.float32) * inv * norm_ref[l:l + 1, cols]).astype(jnp.bfloat16)
            return _

        lax.fori_loop(0, chunks, step, 0)

    def gates(l):
        logits = dot_nt(hbuf[l, ep], router_ref[l])
        ids = lax.broadcasted_iota(jnp.int32, logits.shape, 1)
        p = [jnp.sum(jnp.where(ids == routes_ref[l, :, j:j + 1], logits, 0.0), axis=1, keepdims=True) for j in range(2)]
        top = jnp.maximum(p[0], p[1])
        e = [jnp.exp(p[j] - top) for j in range(2)]
        for j in range(2):
            gates_ref[:, j:j + 1] = e[j] / (e[0] + e[1])

    def source(l, k, f, m):
        i = (l * n_local + k) * MATS + m
        return (weights[m].at[l, k], mate_w.at[i], far_w.at[i], mate_far_w.at[i])[f]

    def up(l, k, q0, nq, service={}):
        with jax.named_scope(f"up#l={l}#k={k}#q={q0}"):
            span = pl.ds(q0 * cap, nq * cap)

            def gu_copies(f):
                return [pltpu.make_async_copy(source(l, k, f, m), wgu.at[f % 2, m], gu_sem.at[f % 2, m]) for m in range(2)]

            for f in range(2):
                for copy in gu_copies(f):
                    copy.start()
            slot_ids = lax.broadcasted_iota(jnp.int32, (cap, tok), 0)
            for q in range(q0, q0 + nq):
                block = xor(ep, q)
                row = ranks[block, pl.ds(l * experts + ep * n_local + k, 1), :].astype(jnp.int32)
                pick = (slot_ids == row).astype(jnp.float32).astype(jnp.bfloat16)

                def pick_cols(c, _, q=q, block=block, pick=pick):
                    cols = cols_of(c)
                    picked[pl.ds(q * cap, cap), cols] = dot(pick, hbuf[l, block, :, cols]).astype(jnp.bfloat16)
                    return _

                lax.fori_loop(0, chunks, pick_cols, 0)

            def up_step(f, _):
                slot = f % 2
                for m in range(2):
                    pltpu.make_async_copy(weights[m].at[l, k], wgu.at[slot, m], gu_sem.at[slot, m]).wait()
                pre_gate = dot_nt(picked[span, :], wgu[slot, 0])
                pre_up = dot_nt(picked[span, :], wgu[slot, 1])
                act[f, span, :] = (jax.nn.silu(pre_gate) * pre_up).astype(jnp.bfloat16)
                for g in range(4):
                    if g < 2 or g in service:
                        @pl.when(f == g)
                        def _(g=g):
                            if g < 2:
                                for copy in gu_copies(g + 2):
                                    copy.start()
                            if g in service:
                                service[g]()
                return 0

            lax.fori_loop(0, 4, up_step, 0)

    def down(l, k, q0, nq):
        with jax.named_scope(f"down#l={l}#k={k}#q={q0}"):
            span = pl.ds(q0 * cap, nq * cap)

            def d_copies(c, slot):
                return [pltpu.make_async_copy(source(l, k, f, 2).at[:, cols_of(c)], wdn.at[slot, f], d_sem.at[slot, f]) for f in range(4)]

            for copy in d_copies(0, 0):
                copy.start()

            def step(c, _):
                slot = c % 2

                @pl.when(c + 1 < chunks)
                def _():
                    for copy in d_copies(jnp.minimum(c + 1, chunks - 1), (c + 1) % 2):
                        copy.start()

                for copy in d_copies(c, slot):
                    copy.wait()
                cols = cols_of(c)
                total = dot(act[0, span, :], wdn[slot, 0])
                for f in range(1, 4):
                    total += dot(act[f, span, :], wdn[slot, f])
                out = total.astype(jnp.bfloat16)
                for n in range(nq):
                    piece = out[n * cap:(n + 1) * cap]
                    if q0 + n == 0:
                        back[k, :, cols] = piece
                    else:
                        outb[(q0 + n - 1) * n_local + k, :, cols] = piece
                return 0

            lax.fori_loop(0, chunks, step, 0)
            for q in range(q0, q0 + nq):
                if q:
                    return_copy(q, k).start()

    def return_copy(q, k):
        j = (q - 1) * n_local + k
        return remote(outb.at[j], back.at[q * n_local + k], rsend.at[j], rrecv.at[j], {"ep": xor(ep, q)})

    def add_part(l, q, k, src_ref, first=False, last=False):
        if q:
            with jax.named_scope(f"return_wait#l={l}#q={q}#k={k}"):
                return_copy(q, k).wait_recv()
        with jax.named_scope(f"add#l={l}#q={q}#k={k}"):
            j = q * n_local + k
            ids = lax.broadcasted_iota(jnp.int32, (tok, cap), 1)
            at = [slots_ref[l, :, c:c + 1] - j * cap for c in range(2)]
            pick = jnp.logical_or(ids == at[0], ids == at[1]).astype(jnp.float32).astype(jnp.bfloat16)
            gate = sum(jnp.where(jnp.logical_and(at[c] >= 0, at[c] < cap), gates_ref[:, c:c + 1], 0.0) for c in range(2))

            def step(c, sq):
                cols = cols_of(c)
                before = src_ref[:, cols].astype(jnp.float32) if first else acc[:, cols]
                after = before + gate * dot(pick, back[j, :, cols])
                if not last:
                    acc[:, cols] = after
                    return sq
                y = after.astype(jnp.bfloat16)
                y_ref[:, cols] = y
                y = y.astype(jnp.float32)
                return sq + jnp.sum(y * y, axis=1, keepdims=True)

            return lax.fori_loop(0, chunks, step, jnp.zeros((tok, 1), jnp.float32))

    def returns_sent():
        for q in range(1, n_ep):
            for k in range(n_local):
                return_copy(q, k).wait_send()

    inner = jnp.logical_and(ep > 0, ep < n_ep - 1)
    outer = jnp.logical_not(inner)
    for i in range(pieces):
        for s in range(2):
            y_copy(i, s).start()
    with jax.named_scope("routing"):
        routing()
    with jax.named_scope("norm0"):
        norm(x_ref, square_sum(x_ref), 0)
    hop_start(0, 1)
    for i in range(pieces):
        m_copy(i).start()
    gates(0)
    pass_x(0, 0)
    pass_x(0, 1)
    pass_x(1, 0)
    pass_mate(0)
    hop_wait(0, 1)
    hop_start(0, 2)
    pass_x(1, 1)
    pass_x(2, 0)
    pass_mate(1)
    weights_ready((0, 1))
    up(0, 0, 0, 2, {1: lambda: pass_x(2, 1)})
    hop_wait(0, 2)
    hop_start(0, 3)
    pass_x(3, 0)
    up(0, 0, 2, 1, {1: lambda: pass_mate(2), 3: lambda: pass_x(3, 1)})
    weights_ready((2,))
    down(0, 0, 2, 1)
    for i in range(pieces, 2 * pieces):
        for s in range(2):
            y_copy(i, s).start()
    down(0, 0, 0, 2)
    pass_x(4, 0)
    pass_mate(3)
    hop_wait(0, 3)
    up(0, 0, 3, 1, {1: lambda: pass_x(4, 1)})
    down(0, 0, 3, 1)
    pass_x(5, 0)
    pass_mate(4)
    weights_ready((3, 4))
    up(0, 1, 0, 4, {1: lambda: pass_x(5, 1), 3: lambda: pass_mate(5)})
    weights_ready((5,))
    down(0, 1, 2, 1)
    pass_x(6, 0)
    down(0, 1, 3, 1)
    down(0, 1, 0, 2)
    pass_x(6, 1)
    for i in range(pieces, 2 * pieces):
        m_copy(i).start()
    add_part(0, 0, 0, x_ref, first=True)
    pass_x(7, 0)
    add_part(0, 0, 1, x_ref)
    add_part(0, 1, 0, x_ref)
    add_part(0, 2, 0, x_ref)
    pass_x(7, 1)
    pass_mate(6)
    pass_x(8, 0)
    add_part(0, 3, 0, x_ref)
    pass_x(8, 1)
    pass_mate(7)
    pass_x(9, 0)
    add_part(0, 1, 1, x_ref)
    add_part(0, 2, 1, x_ref)
    square = add_part(0, 3, 1, x_ref, last=True)
    norm(y_ref, square, 1)
    hop_start(1, 1)
    pass_x(9, 1)
    returns_sent()
    gates(1)
    pass_mate(8)
    pass_x(10, 0)
    pass_x(10, 1)
    pass_mate(9)
    pass_x(11, 0)
    hop_wait(1, 1)
    hop_start(1, 2)
    pass_mate(10)
    weights_ready((6, 7))

    @pl.when(inner)
    def _():
        up(1, 0, 3, 1)
        up(1, 0, 0, 2)

    @pl.when(outer)
    def _():
        up(1, 0, 0, 2)

    pass_x(11, 1)
    weights_ready((8,))

    @pl.when(inner)
    def _():
        down(1, 0, 3, 1)

    down(1, 0, 0, 2)
    hop_wait(1, 2)
    hop_start(1, 3)
    pass_mate(11)
    up(1, 0, 2, 1)
    down(1, 0, 2, 1)
    weights_ready((9, 10))
    up(1, 1, 0, 3)
    weights_ready((11,))
    down(1, 1, 2, 1)

    @pl.when(inner)
    def _():
        up(1, 1, 3, 1)

    @pl.when(outer)
    def _():
        hop_wait(1, 3)
        up(1, 0, 3, 1)
        down(1, 0, 3, 1)
        up(1, 1, 3, 1)

    down(1, 1, 3, 1)
    down(1, 1, 0, 2)
    add_part(1, 0, 0, y_ref, first=True)
    add_part(1, 0, 1, y_ref)
    add_part(1, 1, 0, y_ref)
    add_part(1, 2, 0, y_ref)
    add_part(1, 1, 1, y_ref)
    add_part(1, 2, 1, y_ref)
    add_part(1, 3, 0, y_ref)
    add_part(1, 3, 1, y_ref, last=True)
    returns_sent()
    hop_drain(0)
    hop_drain(1)
    for i in range(2 * pieces):
        for s in range(2):
            y_copy(i, s).wait_send()
            x_copy(i, s).wait_send()
        m_copy(i).wait_send()
        f_copy(i).wait_send()


def moe_layers(x, norm_w, router_t, routes, routes_row, wg, wu, wd, n_ep):
    n_layers, n_local, ff, width = wg.shape
    tok = x.shape[0]
    experts = router_t.shape[1]
    cap = tok // 2
    chunk = min(512, width // 2)
    n = n_layers * n_local * MATS
    bf = jnp.bfloat16
    dma = pltpu.SemaphoreType.DMA
    copies = jax.ShapeDtypeStruct((n, ff, width), bf)
    return pl.pallas_call(
        layers_kernel,
        out_shape=(jax.ShapeDtypeStruct((tok, width), bf), copies, copies, copies),
        in_specs=[VMEM] * 5 + [ANY] * 3, out_specs=(VMEM, ANY, ANY, ANY),
        scratch_shapes=[
            pltpu.VMEM((n_layers, n_ep, tok, width), bf), pltpu.VMEM((n_ep, n_layers * experts, tok), jnp.float32),
            pltpu.VMEM((n_ep * n_local, cap, width), bf), pltpu.VMEM(((n_ep - 1) * n_local, cap, width), bf),
            pltpu.VMEM((n_ep * cap, width), bf), pltpu.VMEM((4, n_ep * cap, ff), bf),
            pltpu.VMEM((2, 2, ff, width), bf), pltpu.VMEM((2, 4, ff, chunk), bf),
            pltpu.VMEM((tok, width), jnp.float32),
            pltpu.VMEM((tok, 2), jnp.float32), pltpu.VMEM((n_layers, tok, 2), jnp.int32),
        ] + [dma((n, 2))] * 4 + [dma((n,))] * 4 + [dma((n_layers, 2, n_ep - 1))] * 2 + [dma((2, n_ep - 1))] * 2
          + [dma(((n_ep - 1) * n_local,))] * 2 + [dma((2, 2)), dma((2, 4))],
        compiler_params=pltpu.CompilerParams(collective_id=0, has_side_effects=True, vmem_limit_bytes=VMEM_BYTES),
        name="moe_layers",
    )(x, norm_w, router_t, routes, routes_row, wg, wu, wd)[0]


def solution(mesh):
    token_spec = P(("rep", "ep", "fsdp"), None)
    expert_in_spec = P(None, "ep", None, "fsdp")
    expert_out_spec = P(None, "ep", "fsdp", None)
    route_spec = P(None, ("rep", "ep", "fsdp"), None)
    n_ep = mesh.shape["ep"]

    def device_step(x_in, norm_w, router_w, gate_w, up_w, down_w, routes):
        return moe_layers(x_in, norm_w, router_w.swapaxes(1, 2), routes, routes.swapaxes(1, 2),
                          gate_w.swapaxes(2, 3), up_w.swapaxes(2, 3), down_w, n_ep)

    return jax.shard_map(device_step, mesh=mesh,
                         in_specs=(token_spec, P(), P(), expert_in_spec, expert_in_spec, expert_out_spec, route_spec),
                         out_specs=token_spec, check_vma=False)
```
